512 devices in a mesh: member: 2 (over y), tile: 128 (over x, z), sub: 2 (over core).
Axes of the slice: x: 8, y: 2, z: 16, core: 2. Of those that a mesh axis runs over, the one named last changes fastest.
The devices are a block of a 8x8x16 slice.
Arguments:
- atm_state: bfloat16 [8, 524288], P(None, ('member', 'tile')), parts along dimension 1, may hold values from -6 to 6
- ocn_state: bfloat16 [4, 524288], P(None, ('member', 'tile', 'sub')), parts along dimension 1, may hold values from -6 to 6
- need_atm: int32 [2048], P(('tile', 'sub')), may hold values from 0 to 2047, as said below
- xb_need: int32 [2048], P(('tile', 'sub')), may hold values from 0 to 15
- xb_ocn: int32 [2048], P(('tile', 'sub')), may hold values from 0 to 15
- xb_count: int32 [256], P(('tile', 'sub')), may hold values from 1 to 8, as said below
- sea_mask: int32 [262144], P(('tile', 'sub')), may hold values 0 or 1
- cell_area: float32 [262144], P(('tile', 'sub')), may hold values from 0.5 to 2
- w_atm: bfloat16 [2048, 128, 128], P(('tile', 'sub')), may hold values from 0.0099487305 to 1
- w_ocn: bfloat16 [2048, 128, 128], P(('tile', 'sub')), may hold values from 0.0099487305 to 1
Outputs:
- atm_flux: float32 [4, 524288], P(None, ('member', 'tile')), parts along dimension 1
- ocn_flux: float32 [4, 524288], P(None, ('member', 'tile', 'sub')), parts along dimension 1
The draws below stay inside these ranges and needn't reach their ends.
There are 2 independent parts, one for each index of `member`. The reference program is written for one: setup_inputs(seed, part) draws one part's arguments, and reference() takes and returns one part's arrays. A program takes and returns all parts, laid end to end along the dimension named above; an argument that names none is the same for every part. Nothing has to cross between parts.
Inputs may be any that keep to these rules, and one draw needn't show every extreme that they name: `need_atm`: an atmosphere block n lies on tile n // 16. A tile's list is the entries of its devices in device order; for tile t its entries 2 i and 2 i + 1 lie on tile (t + i - 8 // 2 + 1) mod 128 for i < 7, and on tile (t + 64) mod 128 for i = 7; all entries of one tile's list are distinct. `xb_need`: index into the list of the block's tile. `xb_ocn`: index among the ocean blocks of the block's tile, in device order. `xb_count`: some device has all 8 blocks live.
All inputs are finite; a program needn't handle non-finite values. No bound on the sum of `sea_mask` on one device may be relied on, other than what follows from the above.
Results may differ from the reference program's by a relative error of at most 0.0003.
Values may be sent and summed in bfloat16 or wider, within the bound.
A program may use at most 64 MiB of HBM per device.

```python
import math
import jax
import jax.numpy as jnp
from jax import lax

F_A = 8
F_O = 4
F_X = 4
BLK = 128
ABLK_TILE = 16
OBLK_DEV = 8
XB_DEV = 8
NEED_DEV = 8
ATM_CELLS = 262144
OCN_CELLS = 262144
XBLKS = 2048
N_TILE = 128
N_SUB = 2


def draw_need_atm(key, part):
    first, second = jax.random.split(key, 2)
    lower = jax.random.randint(first, (N_TILE, NEED_DEV), 0, ABLK_TILE)
    apart = jax.random.randint(second, (N_TILE, NEED_DEV), 1, ABLK_TILE)
    upper = (lower + apart) % ABLK_TILE
    locals_pair = jnp.stack([lower, upper], 2)
    order = jnp.arange(NEED_DEV, dtype=jnp.int32)
    offset = jnp.where(order < NEED_DEV - 1, order - NEED_DEV // 2 + 1, N_TILE // 2)
    owner = (jnp.arange(N_TILE, dtype=jnp.int32)[:, None] + offset[None, :]) % N_TILE
    return (owner[:, :, None] * ABLK_TILE + locals_pair).reshape(-1).astype(jnp.int32)


def draw_xb_count(key, part):
    devices = N_TILE * N_SUB
    shifts = jax.random.randint(key, (devices,), 0, 3)
    chosen = jax.random.randint(jax.random.fold_in(key, 7), (), 0, devices)
    shifts = jnp.where(jnp.arange(devices) == chosen, 0, shifts)
    return (XB_DEV // jnp.left_shift(1, shifts)).astype(jnp.int32)


def with_ends(array, own_key, least, largest):
    dims = array.shape
    place = [jax.random.randint(jax.random.fold_in(own_key, axis), (), 0, dims[axis]) for axis in range(len(dims))]
    array = array.at[tuple(place)].set(least)
    longest = dims.index(max(dims))
    place[longest] = (place[longest] + 1) % dims[longest]
    return array.at[tuple(place)].set(largest)


def block_scale(key, extent, cuts, smallest, top_value):
    level = 1.0
    for position, shards_of in cuts:
        steps = jax.random.uniform(jax.random.fold_in(jax.random.fold_in(key, 6), position), (shards_of,), jnp.float32, smallest / len(cuts), top_value / len(cuts))
        level = level * jnp.repeat(jnp.exp(steps), extent[position] // shards_of).reshape((-1,) + (1,) * (len(extent) - 1 - position))
    return level


def scatter_about(rng, dims, spread, limit, cuts=(), kind=jnp.bfloat16):
    level = block_scale(rng, dims, cuts, -0.22, 0.18) if cuts else 1.0
    entries = jax.random.normal(rng, dims, jnp.float32) * spread * level
    return jnp.minimum(jnp.maximum(entries, -limit), limit).astype(kind)


def setup_inputs(seed: int = 0, part: int = 0) -> dict:
    key_list = jax.random.split(jax.random.key(seed), 11)
    own_keys = jax.random.split(jax.random.fold_in(key_list[10], part), 11)
    return {
        "atm_state": scatter_about(own_keys[0], (F_A, ATM_CELLS), 1.0, 6.0, ((1, 128),)),
        "ocn_state": scatter_about(own_keys[1], (F_O, OCN_CELLS), 1.0, 6.0, ((1, 256),)),
        "need_atm": draw_need_atm(jax.random.fold_in(key_list[10], 71), part),
        "xb_need": with_ends(jax.random.randint(key_list[3], (XBLKS,), 0, N_SUB * NEED_DEV), jax.random.fold_in(key_list[3], 1), 0, (N_SUB * NEED_DEV) - 1).astype(jnp.int32),
        "xb_ocn": with_ends(jax.random.randint(key_list[4], (XBLKS,), 0, N_SUB * OBLK_DEV), jax.random.fold_in(key_list[4], 1), 0, (N_SUB * OBLK_DEV) - 1).astype(jnp.int32),
        "xb_count": draw_xb_count(jax.random.fold_in(key_list[10], 71), part),
        "sea_mask": with_ends((jax.random.randint(key_list[6], (XBLKS * BLK,), 0, 3) < 2).astype(jnp.int32), jax.random.fold_in(key_list[6], 1), 0, 1),
        "cell_area": jnp.clip(jnp.exp(math.log(2.0) - 1.3862944 * jax.random.uniform(key_list[7], (XBLKS * BLK,), jnp.float32) ** block_scale(key_list[7], (XBLKS * BLK,), ((0, 256),), -0.2, 0.2)), 0.5, 2.0),
        "w_atm": jnp.clip(jnp.exp(math.log(1.0) - 4.61031033 * jax.random.uniform(key_list[8], (XBLKS, BLK, BLK), jnp.float32) ** block_scale(key_list[8], (XBLKS, BLK, BLK), ((0, 256),), -0.2, 0.2)), 0.0099487305, 1.0).astype(jnp.bfloat16),
        "w_ocn": jnp.clip(jnp.exp(math.log(1.0) - 4.61031033 * jax.random.uniform(key_list[9], (XBLKS, BLK, BLK), jnp.float32) ** block_scale(key_list[9], (XBLKS, BLK, BLK), ((0, 256),), -0.2, 0.2)), 0.0099487305, 1.0).astype(jnp.bfloat16),
    }


def bulk_fluxes(upper_domain_vector, marine_regrid_transfer):
    lowest_level_warmth, vapour_mixing_ratio, eastward_wind, northward_wind, ground_level_pressure, solar_radiation, infrared_radiation, rainfall_rate = [upper_domain_vector[:, grid_box_number] for grid_box_number in range(8)]
    skin_warmth_kelvin, eastward_current, northward_current, marine_climate_coupler = [marine_regrid_transfer[:, grid_box_number] for grid_box_number in range(4)]
    du = eastward_wind - eastward_current
    dv = northward_wind - northward_current
    speed = jnp.sqrt(du * du + dv * dv + 1.0)
    momentum_transfer_factor = (0.3 + 0.1 * jnp.tanh(ground_level_pressure)) * speed
    conductive_energy_loss = momentum_transfer_factor * (skin_warmth_kelvin - lowest_level_warmth)
    evaporative_energy_loss = momentum_transfer_factor * (0.5 * skin_warmth_kelvin - vapour_mixing_ratio)
    taux = momentum_transfer_factor * du
    tauy = momentum_transfer_factor * dv
    reflected_fraction = 0.06 + 0.1 * jax.nn.sigmoid(marine_climate_coupler)
    thermal_energy_transfer = (1.0 - reflected_fraction) * solar_radiation + infrared_radiation - 0.2 * skin_warmth_kelvin - conductive_energy_loss - evaporative_energy_loss
    fresh = rainfall_rate - 0.5 * evaporative_energy_loss
    return (jnp.stack([conductive_energy_loss, evaporative_energy_loss, taux, tauy], 1), jnp.stack([thermal_energy_transfer, taux, tauy, fresh], 1))

def reference(atm_state, ocn_state, need_atm, xb_need, xb_ocn, xb_count, sea_mask, cell_area, w_atm, w_ocn):
    devices = N_TILE * N_SUB
    highest = lax.Precision.HIGHEST
    atm_table = jnp.transpose(atm_state.reshape(F_A, N_TILE * ABLK_TILE, BLK), (1, 0, 2))
    ocn_table = jnp.transpose(ocn_state.reshape(F_O, devices * OBLK_DEV, BLK), (1, 0, 2))
    list_len = N_SUB * NEED_DEV
    items = (jnp.arange(devices, dtype=jnp.int32), xb_need.reshape(devices, XB_DEV), xb_ocn.reshape(devices, XB_DEV), xb_count, sea_mask.reshape(devices, XB_DEV, BLK), cell_area.reshape(devices, XB_DEV, BLK), w_atm.reshape(devices, XB_DEV, BLK, BLK), w_ocn.reshape(devices, XB_DEV, BLK, BLK))

    def step(carry, item):
        acc_atm, acc_ocn = carry
        device, need_idx, ocn_idx, count, sea, area, weight_a, weight_o = item
        tile = device // N_SUB
        tile_list = lax.dynamic_slice_in_dim(need_atm, (tile * list_len).astype(jnp.int32), list_len)
        ids = tile_list[need_idx]
        oids = (tile * (N_SUB * OBLK_DEV) + ocn_idx).astype(jnp.int32)
        wa = weight_a.astype(jnp.float32)
        wo = weight_o.astype(jnp.float32)
        upper_domain_vector = jnp.einsum('bfj,bxj->bfx', atm_table[ids].astype(jnp.float32), wa, precision=highest) / lax.optimization_barrier(jnp.sum(wa, 2))[:, None, :]
        marine_regrid_transfer = jnp.einsum('bfj,bxj->bfx', ocn_table[oids].astype(jnp.float32), wo, precision=highest) / lax.optimization_barrier(jnp.sum(wo, 2))[:, None, :]
        to_atm, to_ocn = bulk_fluxes(upper_domain_vector, marine_regrid_transfer)
        live = (jnp.arange(XB_DEV, dtype=jnp.int32) < count).astype(jnp.float32)[:, None]
        weighted = area * live
        wet = weighted * sea.astype(jnp.float32)
        atm_terms = jnp.concatenate([to_atm * wet[:, None, :], weighted[:, None, :]], 1)
        ocn_terms = jnp.concatenate([to_ocn * wet[:, None, :], wet[:, None, :]], 1)
        atm_cells = jnp.einsum('bgx,bxj->bgj', atm_terms, wa, precision=highest)
        ocn_cells = jnp.einsum('bgx,bxj->bgj', ocn_terms, wo, precision=highest)
        return ((acc_atm.at[ids].add(atm_cells), acc_ocn.at[oids].add(ocn_cells)), None)
    init = (jnp.zeros((N_TILE * ABLK_TILE, F_X + 1, BLK), jnp.float32), jnp.zeros((devices * OBLK_DEV, F_X + 1, BLK), jnp.float32))
    (acc_atm, acc_ocn), _ = lax.scan(step, init, items)
    atm_flux = acc_atm[:, :F_X] / jnp.maximum(acc_atm[:, F_X:], 1.0)
    ocn_flux = acc_ocn[:, :F_X] / jnp.maximum(acc_ocn[:, F_X:], 1.0)
    atm_flux = jnp.transpose(atm_flux, (1, 0, 2)).reshape(F_X, N_TILE * ABLK_TILE * BLK)
    ocn_flux = jnp.transpose(ocn_flux, (1, 0, 2)).reshape(F_X, devices * OBLK_DEV * BLK)
    return (atm_flux, ocn_flux)
```

```python
import functools

import jax
import jax.numpy as jnp
from jax import lax
from jax.experimental import pallas as pl
from jax.experimental.pallas import tpu as pltpu
from jax.sharding import PartitionSpec as P

MESH = pl.DeviceIdType.MESH
F32 = jnp.float32
BF16 = jnp.bfloat16


def owner_offset(index, npairs, ntile):
    if index < npairs - 1:
        return index - npairs // 2 + 1
    return ntile // 2


def dot_nt(left, right):
    return lax.dot_general(left, right, (((1,), (1,)), ((), ())), preferred_element_type=F32)


def dot_nn(left, right):
    return jnp.dot(left, right, preferred_element_type=F32)


def split(value):
    high = value.astype(BF16).astype(F32)
    return high, value - high


def bulk_fluxes(ta, qa, ua, va, ps, sw, lw, pr, sst, uo, vo, albedo):
    du = ua - uo
    dv = va - vo
    factor = (0.3 + 0.1 * jnp.tanh(ps)) * jnp.sqrt(du * du + dv * dv + 1.0)
    sens = factor * (sst - ta)
    lat = factor * (0.5 * sst - qa)
    taux = factor * du
    tauy = factor * dv
    heat = (1.0 - albedo) * sw + lw - 0.2 * sst - sens - lat
    fresh = pr - 0.5 * lat
    return (sens, lat, taux, tauy), (heat, taux, tauy, fresh)


def kernel(
    ntile,
    npairs,
    atm_hbm,
    ocn_hbm,
    need_hbm,
    xneed_hbm,
    xocn_hbm,
    count_hbm,
    sea_hbm,
    area_hbm,
    wa_hbm,
    wo_hbm,
    atm_out,
    ocn_out,
    need_s,
    xneed_s,
    xocn_s,
    count_s,
    table,
    ocean,
    sea_v,
    area_v,
    wa,
    wo,
    field_a,
    field_o,
    sums_a,
    terms,
    note_out,
    note_in,
    place,
    inverse,
    back_out,
    back_in,
    sea_out,
    sea_in,
    local_sem,
    list_sem,
    ocean_sem,
    push_send,
    push_recv,
    pass_send,
    pass_recv,
    note_send,
    note_recv,
    back_send,
    back_recv,
    final_sem,
):
    tile = lax.axis_index("tile")
    core = lax.axis_index("sub")
    other = 1 - core
    nblocks, blk = wa.shape[0], wa.shape[2]
    owned = table.shape[0] // npairs
    part = owned // 2
    mine = npairs // 2 - 1
    order = [i for i in sorted(range(npairs), key=lambda i: -abs(owner_offset(i, npairs, ntile))) if i != mine]

    def asker(index):
        return lax.rem(tile + 2 * ntile - owner_offset(index, npairs, ntile), ntile)

    def owner(index):
        return lax.rem(tile + ntile + owner_offset(index, npairs, ntile), ntile)

    def remote(source, target, send, recv, where):
        return pltpu.make_async_remote_copy(
            src_ref=source, dst_ref=target, send_sem=send, recv_sem=recv, device_id=where, device_id_type=MESH
        )

    barrier = pltpu.get_barrier_semaphore()
    for index in order:
        for side in range(2):
            pl.semaphore_signal(barrier, inc=1, device_id={"tile": owner(index), "sub": side}, device_id_type=MESH)
    pl.semaphore_signal(barrier, inc=1, device_id={"sub": other}, device_id_type=MESH)

    sources = (atm_hbm, need_hbm, ocn_hbm, xneed_hbm, xocn_hbm, count_hbm, sea_hbm, area_hbm, wa_hbm, wo_hbm)
    targets = (
        table.at[pl.ds(mine * owned, owned)],
        need_s.at[core],
        ocean.at[pl.ds(core * part, part)],
        xneed_s,
        xocn_s,
        count_s,
        sea_v,
        area_v,
        wa,
        wo,
    )
    local = [
        pltpu.make_async_copy(source, target, local_sem.at[i])
        for i, (source, target) in enumerate(zip(sources, targets))
    ]
    for copy in local:
        copy.start()
    local[0].wait()
    local[1].wait()
    local[2].wait()
    pl.semaphore_wait(barrier, 2 * len(order) + 1)

    pushes = {}
    for index in order:
        pushes[index] = remote(
            table.at[pl.ds(mine * owned + core * part, part)],
            table.at[pl.ds(index * owned + core * part, part)],
            push_send.at[index],
            push_recv.at[index],
            {"tile": asker(index)},
        )
        pushes[index].start()
    lists = remote(need_s.at[core], need_s.at[core], list_sem.at[0], list_sem.at[1], {"sub": other})
    lists.start()
    waters = remote(
        ocean.at[pl.ds(core * part, part)],
        ocean.at[pl.ds(core * part, part)],
        ocean_sem.at[0],
        ocean_sem.at[1],
        {"sub": other},
    )
    waters.start()
    for copy in local[3:]:
        copy.wait()

    rows = lax.broadcasted_iota(jnp.int32, (8, blk), 0)
    live = (lax.broadcasted_iota(jnp.int32, (nblocks, blk), 0) < count_s[0]).astype(F32)
    weighted = area_v[...] * live
    wet = weighted * sea_v[...].astype(F32)

    high, low = split(weighted)
    near = jnp.zeros((8, blk), F32)
    far = jnp.zeros((8, blk), F32)
    for b in range(nblocks):
        left = jnp.concatenate(
            [jnp.broadcast_to(high[b : b + 1], (8, blk)), jnp.broadcast_to(low[b : b + 1], (8, blk))], 0
        ).astype(BF16)
        cells = dot_nn(left, wa[b])
        cells = cells[:8] + cells[8:]
        near = near + jnp.where(rows == xneed_s[b], cells, 0.0)
        far = far + jnp.where(rows + 8 == xneed_s[b], cells, 0.0)
    lists.wait()
    for index in range(npairs):
        held = near if index < npairs // 2 else far
        at = (2 * index) % 8
        note_out[index, 0:2] = held[at : at + 2]
        for k in range(2):
            entry = 2 * index + k
            local_block = need_s[entry // 8, entry % 8] & (owned - 1)
            note_out[index, 2 + k : 3 + k] = jnp.full((1, blk), local_block, jnp.int32).astype(F32)
    notes = {}
    for index in order:
        for side in range(2):
            notes[index, side] = remote(
                note_out.at[index],
                note_in.at[index, core],
                note_send.at[index, side],
                note_recv.at[index, core],
                {"tile": owner(index), "sub": side},
            )
            notes[index, side].start()
    note_near = remote(
        note_out.at[mine],
        note_in.at[mine, core],
        note_send.at[mine, 0],
        note_recv.at[mine, core],
        {"sub": other},
    )
    note_near.start()
    note_in[mine, core] = note_out[mine]

    waters.wait()
    for b in range(nblocks):
        state = ocean[xocn_s[b]].astype(F32)
        left = jnp.concatenate([state, jnp.ones((8 - state.shape[0], blk), F32)], 0).astype(BF16)
        field_o[b] = dot_nt(left, wo[b])
    for b in range(nblocks):
        sums_a[b] = dot_nt(jnp.ones((8, blk), BF16), wa[b])
    per_ocean = 1.0 / field_o[:, 4, :]
    per_atm = 1.0 / sums_a[:, 0, :]
    sst = field_o[:, 0, :] * per_ocean
    uo = field_o[:, 1, :] * per_ocean
    vo = field_o[:, 2, :] * per_ocean
    albedo = 0.06 + 0.1 * jax.nn.sigmoid(field_o[:, 3, :] * per_ocean)

    passes = {}
    for index in order:
        pushes[index].wait_recv()
        half = table.at[pl.ds(index * owned + core * part, part)]
        passes[index] = remote(half, half, pass_send.at[index], pass_recv.at[index], {"sub": other})
        passes[index].start()
    for index in order:
        passes[index].wait_recv()

    for b in range(nblocks):
        entry = xneed_s[b]
        block = need_s[entry >> 3, entry & 7] & (owned - 1)
        field_a[b] = dot_nt(table[(entry >> 1) * owned + block], wa[b])
    states = [field_a[:, f, :] * per_atm for f in range(8)]
    to_atm, to_ocn = bulk_fluxes(*states, sst, uo, vo, albedo)
    for g in range(4):
        high, low = split(to_atm[g] * wet)
        terms[:, g, :] = high
        terms[:, g + 4, :] = high
        terms[:, g + 8, :] = low
        terms[:, g + 12, :] = low
    lower = (rows >= 4).astype(jnp.int32)
    pairs = [jnp.zeros((8, blk), F32) for _ in range(npairs)]
    for b in range(nblocks):
        cells = dot_nn(terms[b].astype(BF16), wa[b])
        cells = cells[:8] + cells[8:]
        entry = xneed_s[b] - lower
        for index in range(npairs):
            pairs[index] = pairs[index] + jnp.where(entry == 2 * index, cells, 0.0)
    for index in range(npairs):
        back_out[index] = pairs[index]
    backs = {}
    for index in order:
        for side in range(2):
            backs[index, side] = remote(
                back_out.at[index],
                back_in.at[index, core],
                back_send.at[index, side],
                back_recv.at[index, core],
                {"tile": owner(index), "sub": side},
            )
            backs[index, side].start()
    back_near = remote(
        back_out.at[mine],
        back_in.at[mine, core],
        back_send.at[mine, 0],
        back_recv.at[mine, core],
        {"sub": other},
    )
    back_near.start()
    back_in[mine, core] = pairs[mine]

    for g in range(5):
        high, low = split(to_ocn[g] * wet if g < 4 else wet)
        terms[:, g, :] = high
        terms[:, g + 8, :] = low
    for g in range(5, 8):
        terms[:, g, :] = jnp.zeros((nblocks, blk), F32)
        terms[:, g + 8, :] = jnp.zeros((nblocks, blk), F32)
    sums = [jnp.zeros((8, blk), F32) for _ in range(2 * part)]
    for b in range(nblocks):
        cells = dot_nn(terms[b].astype(BF16), wo[b])
        cells = cells[:8] + cells[8:]
        entry = jnp.full((8, blk), xocn_s[b], jnp.int32)
        for index in range(2 * part):
            sums[index] = sums[index] + jnp.where(entry == index, cells, 0.0)
    for index in range(2 * part):
        sea_out[index // part, index % part] = sums[index]
    shore = remote(sea_out.at[other], sea_in, final_sem.at[0], final_sem.at[1], {"sub": other})
    shore.start()

    for index in order:
        for side in range(2):
            remote(
                note_out.at[index],
                note_in.at[index, side],
                note_send.at[index, side],
                note_recv.at[index, side],
                {"tile": owner(index), "sub": side},
            ).wait_recv()
    remote(
        note_out.at[mine],
        note_in.at[mine, other],
        note_send.at[mine, 0],
        note_recv.at[mine, other],
        {"sub": other},
    ).wait_recv()
    areas = []
    spots = []
    for index in range(npairs):
        areas.append(note_in[index, 0, 0:2] + note_in[index, 1, 0:2])
        spot = note_in[index, 0, 2:4]
        spots.append(spot)
        place[index] = jnp.concatenate(
            [jnp.broadcast_to(spot[0:1], (4, blk)), jnp.broadcast_to(spot[1:2], (4, blk))], 0
        )
    areas = jnp.concatenate(areas, 0)
    spots = jnp.concatenate(spots, 0)
    for a in range(owned):
        total = jnp.sum(jnp.where(spots == float(a), areas, 0.0), 0, keepdims=True)
        inverse[a : a + 1] = 1.0 / jnp.maximum(total, 1.0)

    shore.wait_recv()
    for m in range(part):
        total = sea_out[core, m] + sea_in[m]
        ocn_out[m] = total[:4] / jnp.maximum(total[4:5], 1.0)

    for index in order:
        for side in range(2):
            remote(
                back_out.at[index],
                back_in.at[index, side],
                back_send.at[index, side],
                back_recv.at[index, side],
                {"tile": owner(index), "sub": side},
            ).wait_recv()
    remote(
        back_out.at[mine],
        back_in.at[mine, other],
        back_send.at[mine, 0],
        back_recv.at[mine, other],
        {"sub": other},
    ).wait_recv()
    pairs = [back_in[index, 0] + back_in[index, 1] for index in range(npairs)]
    for a in range(owned):
        total = jnp.zeros((8, blk), F32)
        for index in range(npairs):
            total = total + jnp.where(place[index] == float(a), pairs[index], 0.0)
        atm_out[a] = (total[:4] + total[4:]) * inverse[a : a + 1]

    for index in order:
        pushes[index].wait_send()
        passes[index].wait_send()
        for side in range(2):
            notes[index, side].wait_send()
            backs[index, side].wait_send()
    note_near.wait_send()
    back_near.wait_send()
    shore.wait_send()


def per_device(atm_state, ocn_state, need_atm, xb_need, xb_ocn, xb_count, sea_mask, cell_area, w_atm, w_ocn):
    ntile = lax.axis_size("tile")
    fields_a = atm_state.shape[0]
    fields_o = ocn_state.shape[0]
    nblocks, blk = w_atm.shape[0], w_atm.shape[1]
    npairs = need_atm.shape[0]
    owned = atm_state.shape[1] // blk
    waters = ocn_state.shape[1] // blk
    nflux = 4
    atm = jnp.transpose(atm_state.reshape(fields_a, owned, blk), (1, 0, 2))
    ocn = jnp.transpose(ocn_state.reshape(fields_o, waters, blk), (1, 0, 2))
    dma = pltpu.SemaphoreType.DMA
    vmem = pltpu.VMEM
    atm_flux, ocn_flux = pl.pallas_call(
        functools.partial(kernel, ntile, npairs),
        out_shape=(
            jax.ShapeDtypeStruct((owned, nflux, blk), F32),
            jax.ShapeDtypeStruct((waters, nflux, blk), F32),
        ),
        in_specs=[pl.BlockSpec(memory_space=pl.ANY)] * 10,
        out_specs=[pl.BlockSpec(memory_space=pltpu.VMEM)] * 2,
        scratch_shapes=[
            pltpu.SMEM((2, npairs), jnp.int32),
            pltpu.SMEM((nblocks,), jnp.int32),
            pltpu.SMEM((nblocks,), jnp.int32),
            pltpu.SMEM((1,), jnp.int32),
            vmem((npairs * owned, fields_a, blk), BF16),
            vmem((2 * waters, fields_o, blk), BF16),
            vmem((nblocks, blk), jnp.int32),
            vmem((nblocks, blk), F32),
            vmem((nblocks, blk, blk), BF16),
            vmem((nblocks, blk, blk), BF16),
            vmem((nblocks, 8, blk), F32),
            vmem((nblocks, 8, blk), F32),
            vmem((nblocks, 8, blk), F32),
            vmem((nblocks, 16, blk), F32),
            vmem((npairs, 4, blk), F32),
            vmem((npairs, 2, 4, blk), F32),
            vmem((npairs, 8, blk), F32),
            vmem((owned, blk), F32),
            vmem((npairs, 8, blk), F32),
            vmem((npairs, 2, 8, blk), F32),
            vmem((2, waters, 8, blk), F32),
            vmem((waters, 8, blk), F32),
            dma((10,)),
            dma((2,)),
            dma((2,)),
            dma((npairs,)),
            dma((npairs,)),
            dma((npairs,)),
            dma((npairs,)),
            dma((npairs, 2)),
            dma((npairs, 2)),
            dma((npairs, 2)),
            dma((npairs, 2)),
            dma((2,)),
        ],
        compiler_params=pltpu.CompilerParams(collective_id=0, has_side_effects=True),
    )(
        atm,
        ocn,
        need_atm,
        xb_need,
        xb_ocn,
        xb_count,
        sea_mask.reshape(nblocks, blk),
        cell_area.reshape(nblocks, blk),
        w_atm,
        w_ocn,
    )
    atm_flux = jnp.transpose(atm_flux, (1, 0, 2)).reshape(nflux, owned * blk)
    ocn_flux = jnp.transpose(ocn_flux, (1, 0, 2)).reshape(nflux, waters * blk)
    return (atm_flux, ocn_flux)


def solution(mesh):
    placed = (
        P(None, ("member", "tile")),
        P(None, ("member", "tile", "sub")),
        P(("tile", "sub")),
        P(("tile", "sub")),
        P(("tile", "sub")),
        P(("tile", "sub")),
        P(("tile", "sub")),
        P(("tile", "sub")),
        P(("tile", "sub"), None, None),
        P(("tile", "sub"), None, None),
    )
    return jax.shard_map(
        per_device,
        mesh=mesh,
        in_specs=placed,
        out_specs=(P(None, ("member", "tile")), P(None, ("member", "tile", "sub"))),
        check_vma=False,
    )
```

```python
import functools

import jax
import jax.numpy as jnp
from jax import lax
from jax.experimental import pallas as pl
from jax.experimental.pallas import tpu as pltpu
from jax.sharding import PartitionSpec as P

MESH = pl.DeviceIdType.MESH
F32 = jnp.float32
BF16 = jnp.bfloat16
VMEM_LIMIT = 60 << 20
LANDING_LIMIT = 4 << 20


def owner_offset(index, npairs, ntile):
    if index < npairs - 1:
        return index - npairs // 2 + 1
    return ntile // 2


def dot_nt(left, right):
    return lax.dot_general(left, right, (((1,), (1,)), ((), ())), preferred_element_type=F32)


def dot_nn(left, right):
    return jnp.dot(left, right, preferred_element_type=F32)


def split(value):
    high = value.astype(BF16).astype(F32)
    return high, value - high


def bulk_fluxes(ta, qa, ua, va, ps, sw, lw, pr, sst, uo, vo, albedo):
    du = ua - uo
    dv = va - vo
    factor = (0.3 + 0.1 * jnp.tanh(ps)) * jnp.sqrt(du * du + dv * dv + 1.0)
    sens = factor * (sst - ta)
    lat = factor * (0.5 * sst - qa)
    taux = factor * du
    tauy = factor * dv
    heat = (1.0 - albedo) * sw + lw - 0.2 * sst - sens - lat
    fresh = pr - 0.5 * lat
    return (sens, lat, taux, tauy), (heat, taux, tauy, fresh)


def kernel(
    ntile,
    npairs,
    atm_hbm,
    ocn_hbm,
    need_hbm,
    xneed_hbm,
    xocn_hbm,
    count_hbm,
    sea_hbm,
    area_hbm,
    wa_hbm,
    wo_hbm,
    back_in,
    place,
    inverse,
    ocn_out,
    need_s,
    xneed_s,
    xocn_s,
    count_s,
    table,
    ocean,
    sea_v,
    area_v,
    wa,
    wo,
    field_a,
    field_o,
    sums_a,
    terms,
    note_out,
    note_in,
    back_out,
    sea_out,
    sea_in,
    local_sem,
    list_sem,
    ocean_sem,
    push_send,
    push_recv,
    pass_send,
    pass_recv,
    note_send,
    note_recv,
    back_send,
    back_recv,
    final_sem,
):
    tile = lax.axis_index("tile")
    core = lax.axis_index("sub")
    other = 1 - core
    nblocks, blk = wa.shape[0], wa.shape[2]
    owned = table.shape[0] // npairs
    part = owned // 2
    mine = npairs // 2 - 1
    order = [i for i in sorted(range(npairs), key=lambda i: -abs(owner_offset(i, npairs, ntile))) if i != mine]

    def asker(index):
        return lax.rem(tile + 2 * ntile - owner_offset(index, npairs, ntile), ntile)

    def owner(index):
        return lax.rem(tile + ntile + owner_offset(index, npairs, ntile), ntile)

    def remote(source, target, send, recv, where):
        return pltpu.make_async_remote_copy(
            src_ref=source, dst_ref=target, send_sem=send, recv_sem=recv, device_id=where, device_id_type=MESH
        )

    barrier = pltpu.get_barrier_semaphore()
    for index in order:
        for side in range(2):
            pl.semaphore_signal(barrier, inc=1, device_id={"tile": owner(index), "sub": side}, device_id_type=MESH)
    pl.semaphore_signal(barrier, inc=1, device_id={"sub": other}, device_id_type=MESH)

    sources = (atm_hbm, need_hbm, ocn_hbm, xneed_hbm, xocn_hbm, count_hbm, sea_hbm, area_hbm, wa_hbm, wo_hbm)
    targets = (
        table.at[pl.ds(mine * owned, owned)],
        need_s.at[core],
        ocean.at[pl.ds(core * part, part)],
        xneed_s,
        xocn_s,
        count_s,
        sea_v,
        area_v,
        wa,
        wo,
    )
    local = [
        pltpu.make_async_copy(source, target, local_sem.at[i])
        for i, (source, target) in enumerate(zip(sources, targets))
    ]
    for copy in local:
        copy.start()
    local[0].wait()
    local[1].wait()
    local[2].wait()
    pl.semaphore_wait(barrier, 2 * len(order) + 1)

    pushes = {}
    for index in order:
        pushes[index] = remote(
            table.at[pl.ds(mine * owned + core * part, part)],
            table.at[pl.ds(index * owned + core * part, part)],
            push_send.at[index],
            push_recv.at[index],
            {"tile": asker(index)},
        )
        pushes[index].start()
    lists = remote(need_s.at[core], need_s.at[core], list_sem.at[0], list_sem.at[1], {"sub": other})
    lists.start()
    waters = remote(
        ocean.at[pl.ds(core * part, part)],
        ocean.at[pl.ds(core * part, part)],
        ocean_sem.at[0],
        ocean_sem.at[1],
        {"sub": other},
    )
    waters.start()
    for copy in local[3:]:
        copy.wait()

    rows = lax.broadcasted_iota(jnp.int32, (8, blk), 0)
    live = (lax.broadcasted_iota(jnp.int32, (nblocks, blk), 0) < count_s[0]).astype(F32)
    weighted = area_v[...] * live
    wet = weighted * sea_v[...].astype(F32)

    high, low = split(weighted)
    near = jnp.zeros((8, blk), F32)
    far = jnp.zeros((8, blk), F32)
    for b in range(nblocks):
        left = jnp.concatenate(
            [jnp.broadcast_to(high[b : b + 1], (8, blk)), jnp.broadcast_to(low[b : b + 1], (8, blk))], 0
        ).astype(BF16)
        cells = dot_nn(left, wa[b])
        cells = cells[:8] + cells[8:]
        near = near + jnp.where(rows == xneed_s[b], cells, 0.0)
        far = far + jnp.where(rows + 8 == xneed_s[b], cells, 0.0)
    lists.wait()
    for index in range(npairs):
        held = near if index < npairs // 2 else far
        at = (2 * index) % 8
        note_out[index, 0:2] = held[at : at + 2]
        for k in range(2):
            entry = 2 * index + k
            local_block = need_s[entry // 8, entry % 8] & (owned - 1)
            note_out[index, 2 + k : 3 + k] = jnp.full((1, blk), local_block, jnp.int32).astype(F32)
    notes = {}
    for index in order:
        for side in range(2):
            notes[index, side] = remote(
                note_out.at[index],
                note_in.at[index, core],
                note_send.at[index, side],
                note_recv.at[index, core],
                {"tile": owner(index), "sub": side},
            )
            notes[index, side].start()
    note_near = remote(
        note_out.at[mine],
        note_in.at[mine, core],
        note_send.at[mine, 0],
        note_recv.at[mine, core],
        {"sub": other},
    )
    note_near.start()
    note_in[mine, core] = note_out[mine]

    waters.wait()
    for b in range(nblocks):
        state = ocean[xocn_s[b]].astype(F32)
        left = jnp.concatenate([state, jnp.ones((8 - state.shape[0], blk), F32)], 0).astype(BF16)
        field_o[b] = dot_nt(left, wo[b])
    for b in range(nblocks):
        sums_a[b] = dot_nt(jnp.ones((8, blk), BF16), wa[b])
    per_ocean = 1.0 / field_o[:, 4, :]
    per_atm = 1.0 / sums_a[:, 0, :]
    sst = field_o[:, 0, :] * per_ocean
    uo = field_o[:, 1, :] * per_ocean
    vo = field_o[:, 2, :] * per_ocean
    albedo = 0.06 + 0.1 * jax.nn.sigmoid(field_o[:, 3, :] * per_ocean)

    passes = {}
    for index in order:
        pushes[index].wait_recv()
        half = table.at[pl.ds(index * owned + core * part, part)]
        passes[index] = remote(half, half, pass_send.at[index], pass_recv.at[index], {"sub": other})
        passes[index].start()
    for index in order:
        passes[index].wait_recv()

    for b in range(nblocks):
        entry = xneed_s[b]
        block = need_s[entry >> 3, entry & 7] & (owned - 1)
        field_a[b] = dot_nt(table[(entry >> 1) * owned + block], wa[b])
    states = [field_a[:, f, :] * per_atm for f in range(8)]
    to_atm, to_ocn = bulk_fluxes(*states, sst, uo, vo, albedo)
    for g in range(4):
        high, low = split(to_atm[g] * wet)
        terms[:, g, :] = high
        terms[:, g + 4, :] = high
        terms[:, g + 8, :] = low
        terms[:, g + 12, :] = low
    lower = (rows >= 4).astype(jnp.int32)
    pairs = [jnp.zeros((8, blk), F32) for _ in range(npairs)]
    for b in range(nblocks):
        cells = dot_nn(terms[b].astype(BF16), wa[b])
        cells = cells[:8] + cells[8:]
        entry = xneed_s[b] - lower
        for index in range(npairs):
            pairs[index] = pairs[index] + jnp.where(entry == 2 * index, cells, 0.0)
    for index in range(npairs):
        back_out[index] = pairs[index]
    backs = {}
    for index in order:
        for side in range(2):
            backs[index, side] = remote(
                back_out.at[index],
                back_in.at[index, core],
                back_send.at[index, side],
                back_recv.at[index, core],
                {"tile": owner(index), "sub": side},
            )
            backs[index, side].start()
    back_near = remote(
        back_out.at[mine],
        back_in.at[mine, core],
        back_send.at[mine, 0],
        back_recv.at[mine, core],
        {"sub": other},
    )
    back_near.start()
    back_in[mine, core] = pairs[mine]

    for g in range(5):
        high, low = split(to_ocn[g] * wet if g < 4 else wet)
        terms[:, g, :] = high
        terms[:, g + 8, :] = low
    for g in range(5, 8):
        terms[:, g, :] = jnp.zeros((nblocks, blk), F32)
        terms[:, g + 8, :] = jnp.zeros((nblocks, blk), F32)
    sums = [jnp.zeros((8, blk), F32) for _ in range(2 * part)]
    for b in range(nblocks):
        cells = dot_nn(terms[b].astype(BF16), wo[b])
        cells = cells[:8] + cells[8:]
        entry = jnp.full((8, blk), xocn_s[b], jnp.int32)
        for index in range(2 * part):
            sums[index] = sums[index] + jnp.where(entry == index, cells, 0.0)
    for index in range(2 * part):
        sea_out[index // part, index % part] = sums[index]
    shore = remote(sea_out.at[other], sea_in, final_sem.at[0], final_sem.at[1], {"sub": other})
    shore.start()

    for index in order:
        for side in range(2):
            remote(
                note_out.at[index],
                note_in.at[index, side],
                note_send.at[index, side],
                note_recv.at[index, side],
                {"tile": owner(index), "sub": side},
            ).wait_recv()
    remote(
        note_out.at[mine],
        note_in.at[mine, other],
        note_send.at[mine, 0],
        note_recv.at[mine, other],
        {"sub": other},
    ).wait_recv()
    areas = []
    spots = []
    for index in range(npairs):
        areas.append(note_in[index, 0, 0:2] + note_in[index, 1, 0:2])
        spot = note_in[index, 0, 2:4]
        spots.append(spot)
        place[index] = jnp.concatenate(
            [jnp.broadcast_to(spot[0:1], (4, blk)), jnp.broadcast_to(spot[1:2], (4, blk))], 0
        )
    areas = jnp.concatenate(areas, 0)
    spots = jnp.concatenate(spots, 0)
    for a in range(owned):
        total = jnp.sum(jnp.where(spots == float(a), areas, 0.0), 0, keepdims=True)
        inverse[a : a + 1] = 1.0 / jnp.maximum(total, 1.0)

    shore.wait_recv()
    for m in range(part):
        total = sea_out[core, m] + sea_in[m]
        ocn_out[m] = total[:4] / jnp.maximum(total[4:5], 1.0)

    for index in order:
        for side in range(2):
            remote(
                back_out.at[index],
                back_in.at[index, side],
                back_send.at[index, side],
                back_recv.at[index, side],
                {"tile": owner(index), "sub": side},
            ).wait_recv()
    remote(
        back_out.at[mine],
        back_in.at[mine, other],
        back_send.at[mine, 0],
        back_recv.at[mine, other],
        {"sub": other},
    ).wait_recv()

    for index in order:
        pushes[index].wait_send()
        passes[index].wait_send()
        for side in range(2):
            notes[index, side].wait_send()
            backs[index, side].wait_send()
    note_near.wait_send()
    back_near.wait_send()
    shore.wait_send()


def landing(back, place, inverse, ocean, atm_out, ocn_out):
    npairs = back.shape[0]
    pairs = [back[index, 0] + back[index, 1] for index in range(npairs)]
    for a in range(inverse.shape[0]):
        total = jnp.zeros(pairs[0].shape, F32)
        for index in range(npairs):
            total = total + jnp.where(place[index] == float(a), pairs[index], 0.0)
        atm_out[a] = (total[:4] + total[4:]) * inverse[a : a + 1]
    ocn_out[...] = ocean[...]


def per_device(atm_state, ocn_state, need_atm, xb_need, xb_ocn, xb_count, sea_mask, cell_area, w_atm, w_ocn):
    ntile = lax.axis_size("tile")
    fields_a = atm_state.shape[0]
    fields_o = ocn_state.shape[0]
    nblocks, blk = w_atm.shape[0], w_atm.shape[1]
    npairs = need_atm.shape[0]
    owned = atm_state.shape[1] // blk
    waters = ocn_state.shape[1] // blk
    nflux = 4
    atm = jnp.transpose(atm_state.reshape(fields_a, owned, blk), (1, 0, 2))
    ocn = jnp.transpose(ocn_state.reshape(fields_o, waters, blk), (1, 0, 2))
    dma = pltpu.SemaphoreType.DMA
    vmem = pltpu.VMEM
    in_vmem = pl.BlockSpec(memory_space=vmem)
    arrived = pl.pallas_call(
        functools.partial(kernel, ntile, npairs),
        out_shape=(
            vmem((npairs, 2, 8, blk), F32),
            vmem((npairs, 8, blk), F32),
            vmem((owned, blk), F32),
            vmem((waters, nflux, blk), F32),
        ),
        in_specs=[pl.BlockSpec(memory_space=pl.ANY)] * 10,
        out_specs=[in_vmem] * 4,
        scratch_shapes=[
            pltpu.SMEM((2, npairs), jnp.int32),
            pltpu.SMEM((nblocks,), jnp.int32),
            pltpu.SMEM((nblocks,), jnp.int32),
            pltpu.SMEM((1,), jnp.int32),
            vmem((npairs * owned, fields_a, blk), BF16),
            vmem((2 * waters, fields_o, blk), BF16),
            vmem((nblocks, blk), jnp.int32),
            vmem((nblocks, blk), F32),
            vmem((nblocks, blk, blk), BF16),
            vmem((nblocks, blk, blk), BF16),
            vmem((nblocks, 8, blk), F32),
            vmem((nblocks, 8, blk), F32),
            vmem((nblocks, 8, blk), F32),
            vmem((nblocks, 16, blk), F32),
            vmem((npairs, 4, blk), F32),
            vmem((npairs, 2, 4, blk), F32),
            vmem((npairs, 8, blk), F32),
            vmem((2, waters, 8, blk), F32),
            vmem((waters, 8, blk), F32),
            dma((10,)),
            dma((2,)),
            dma((2,)),
            dma((npairs,)),
            dma((npairs,)),
            dma((npairs,)),
            dma((npairs,)),
            dma((npairs, 2)),
            dma((npairs, 2)),
            dma((npairs, 2)),
            dma((npairs, 2)),
            dma((2,)),
        ],
        compiler_params=pltpu.CompilerParams(
            collective_id=0, has_side_effects=True, vmem_limit_bytes=VMEM_LIMIT
        ),
    )(
        atm,
        ocn,
        need_atm,
        xb_need,
        xb_ocn,
        xb_count,
        sea_mask.reshape(nblocks, blk),
        cell_area.reshape(nblocks, blk),
        w_atm,
        w_ocn,
    )
    atm_flux, ocn_flux = pl.pallas_call(
        landing,
        out_shape=(
            jax.ShapeDtypeStruct((owned, nflux, blk), F32),
            jax.ShapeDtypeStruct((waters, nflux, blk), F32),
        ),
        in_specs=[in_vmem] * 4,
        out_specs=[in_vmem] * 2,
        compiler_params=pltpu.CompilerParams(vmem_limit_bytes=LANDING_LIMIT),
    )(*arrived)
    atm_flux = jnp.transpose(atm_flux, (1, 0, 2)).reshape(nflux, owned * blk)
    ocn_flux = jnp.transpose(ocn_flux, (1, 0, 2)).reshape(nflux, waters * blk)
    return (atm_flux, ocn_flux)


def solution(mesh):
    placed = (
        P(None, ("member", "tile")),
        P(None, ("member", "tile", "sub")),
        P(("tile", "sub")),
        P(("tile", "sub")),
        P(("tile", "sub")),
        P(("tile", "sub")),
        P(("tile", "sub")),
        P(("tile", "sub")),
        P(("tile", "sub"), None, None),
        P(("tile", "sub"), None, None),
    )
    return jax.shard_map(
        per_device,
        mesh=mesh,
        in_specs=placed,
        out_specs=(P(None, ("member", "tile")), P(None, ("member", "tile", "sub"))),
        check_vma=False,
    )
```

```python
import functools

import jax
import jax.numpy as jnp
from jax import lax
from jax.experimental import pallas as pl
from jax.experimental.pallas import tpu as pltpu
from jax.sharding import PartitionSpec as P

MESH = pl.DeviceIdType.MESH
F32 = jnp.float32
BF16 = jnp.bfloat16
VMEM_LIMIT = 60 << 20
LANDING_LIMIT = 4 << 20


def owner_offset(index, npairs, ntile):
    if index < npairs - 1:
        return index - npairs // 2 + 1
    return ntile // 2


def dot_nt(left, right):
    return lax.dot_general(left, right, (((1,), (1,)), ((), ())), preferred_element_type=F32)


def dot_nn(left, right):
    return jnp.dot(left, right, preferred_element_type=F32)


def split(value):
    high = value.astype(BF16).astype(F32)
    return high, value - high


def bulk_fluxes(ta, qa, ua, va, ps, sw, lw, pr, sst, uo, vo, albedo):
    du = ua - uo
    dv = va - vo
    factor = (0.3 + 0.1 * jnp.tanh(ps)) * jnp.sqrt(du * du + dv * dv + 1.0)
    sens = factor * (sst - ta)
    lat = factor * (0.5 * sst - qa)
    taux = factor * du
    tauy = factor * dv
    heat = (1.0 - albedo) * sw + lw - 0.2 * sst - sens - lat
    fresh = pr - 0.5 * lat
    return (sens, lat, taux, tauy), (heat, taux, tauy, fresh)


def all_of(ref, sem):
    return pltpu.make_async_copy(ref, ref, sem)


def kernel(
    ntile,
    npairs,
    atm_hbm,
    ocn_hbm,
    need_hbm,
    xneed_hbm,
    xocn_hbm,
    count_hbm,
    sea_hbm,
    area_hbm,
    wa_hbm,
    wo_hbm,
    back_in,
    place,
    inverse,
    ocn_out,
    index_s,
    count_s,
    table,
    ocean,
    sea_v,
    area_v,
    wa,
    wo,
    field_a,
    field_o,
    sums_a,
    terms,
    note_out,
    note_in,
    back_out,
    shore,
    local_sem,
    gift_send,
    gift_recv,
    push_sem,
    note_sem,
    back_sem,
    prep_sem,
):
    tile = lax.axis_index("tile")
    core = lax.axis_index("sub")
    nblocks, blk = wa.shape[0], wa.shape[2]
    half = nblocks // 2
    owned = table.shape[0] // npairs
    mine = npairs // 2 - 1
    order = [i for i in sorted(range(npairs), key=lambda i: -abs(owner_offset(i, npairs, ntile))) if i != mine]
    there = len(order)

    def asker(index):
        return lax.rem(tile + 2 * ntile - owner_offset(index, npairs, ntile), ntile)

    def owner(index):
        return lax.rem(tile + ntile + owner_offset(index, npairs, ntile), ntile)

    def remote(source, target, send, recv, where):
        return pltpu.make_async_remote_copy(
            src_ref=source, dst_ref=target, send_sem=send, recv_sem=recv, device_id=where, device_id_type=MESH
        )

    barrier = pltpu.get_barrier_semaphore()
    lists = (need_hbm, xneed_hbm, xocn_hbm)
    small = ((ocn_hbm, ocean), (sea_hbm, sea_v), (area_hbm, area_v))
    large = ((wa_hbm, wa), (wo_hbm, wo))

    def slot(ref, side):
        return ref.at[pl.ds(side * half, half)]

    @pl.when(core == 0)
    def _():
        pl.semaphore_signal(barrier, inc=1, device_id={"sub": 1}, device_id_type=MESH)
        for row, source in enumerate(lists):
            pltpu.make_async_copy(source, index_s.at[0, row], local_sem.at[1]).start()
        count = pltpu.make_async_copy(count_hbm, count_s.at[0], local_sem.at[2])
        count.start()
        pl.semaphore_wait(barrier, 1)
        for source, target in large:
            remote(source, slot(target, 0), gift_send.at[3], gift_recv.at[3], {"sub": 1}).start()
        for source, target in small:
            remote(source, slot(target, 0), gift_send.at[2], gift_recv.at[2], {"sub": 1}).start()
        all_of(index_s.at[0], local_sem.at[1]).wait()
        count.wait()
        numbers = remote(index_s.at[0], index_s.at[0], gift_send.at[0], gift_recv.at[0], {"sub": 1})
        numbers.start()
        limit = remote(count_s.at[0], count_s.at[0], gift_send.at[1], gift_recv.at[1], {"sub": 1})
        limit.start()
        numbers.wait_send()
        limit.wait_send()
        all_of(ocean, gift_send.at[2]).wait()
        all_of(wa, gift_send.at[3]).wait()
        all_of(field_a.at[pl.ds(0, 14)], prep_sem.at[1]).wait()
        all_of(back_in, back_sem.at[1]).wait()

    @pl.when(core == 1)
    def _():
        for index in order:
            pl.semaphore_signal(barrier, inc=1, device_id={"tile": owner(index)}, device_id_type=MESH)
        pl.semaphore_signal(barrier, inc=1, device_id={"sub": 0}, device_id_type=MESH)
        home = pltpu.make_async_copy(atm_hbm, table.at[pl.ds(mine * owned, owned)], local_sem.at[0])
        home.start()
        for row, source in enumerate(lists):
            pltpu.make_async_copy(source, index_s.at[1, row], local_sem.at[1]).start()
        count = pltpu.make_async_copy(count_hbm, count_s.at[1], local_sem.at[2])
        count.start()
        for source, target in small:
            pltpu.make_async_copy(source, slot(target, 1), local_sem.at[3]).start()
        for source, target in large:
            pltpu.make_async_copy(source, slot(target, 1), local_sem.at[4]).start()
        home.wait()
        pl.semaphore_wait(barrier, there + 1)
        for index in order:
            remote(
                table.at[pl.ds(mine * owned, owned)],
                table.at[pl.ds(index * owned, owned)],
                push_sem.at[0],
                push_sem.at[1],
                {"tile": asker(index)},
            ).start()
        all_of(index_s.at[1], local_sem.at[1]).wait()
        count.wait()
        all_of(ocean, local_sem.at[3]).wait()
        all_of(wa, local_sem.at[4]).wait()
        all_of(index_s.at[0], gift_recv.at[0]).wait()
        all_of(count_s.at[0], gift_recv.at[1]).wait()
        all_of(ocean, gift_recv.at[2]).wait()
        all_of(wa, gift_recv.at[3]).wait()

        def listed(entry):
            return index_s[entry >> 3, 0, entry & 7] & (owned - 1)

        xneed = [index_s[b // half, 1, b % half] for b in range(nblocks)]
        xocn = [index_s[b // half, 2, b % half] for b in range(nblocks)]
        rows = lax.broadcasted_iota(jnp.int32, (8, blk), 0)
        block = lax.broadcasted_iota(jnp.int32, (nblocks, blk), 0)
        live = (block < jnp.where(block < half, count_s[0, 0], half + count_s[1, 0])).astype(F32)
        weighted = area_v[...] * live
        wet = weighted * sea_v[...].astype(F32)

        high, low = split(weighted)
        near = jnp.zeros((8, blk), F32)
        far = jnp.zeros((8, blk), F32)
        for b in range(nblocks):
            left = jnp.concatenate(
                [jnp.broadcast_to(high[b : b + 1], (8, blk)), jnp.broadcast_to(low[b : b + 1], (8, blk))], 0
            ).astype(BF16)
            cells = dot_nn(left, wa[b])
            cells = cells[:8] + cells[8:]
            near = near + jnp.where(rows == xneed[b], cells, 0.0)
            far = far + jnp.where(rows + 8 == xneed[b], cells, 0.0)
        for index in range(npairs):
            held = near if index < npairs // 2 else far
            at = (2 * index) % 8
            note_out[index, 0:2] = held[at : at + 2]
            for k in range(2):
                note_out[index, 2 + k : 3 + k] = jnp.full((1, blk), listed(2 * index + k), jnp.int32).astype(F32)
        for index in order:
            remote(
                note_out.at[index], note_in.at[index], note_sem.at[0], note_sem.at[1], {"tile": owner(index)}
            ).start()

        for b in range(nblocks):
            state = ocean[xocn[b]].astype(F32)
            left = jnp.concatenate([state, jnp.ones((8 - state.shape[0], blk), F32)], 0).astype(BF16)
            field_o[b] = dot_nt(left, wo[b])
        for b in range(nblocks):
            sums_a[b] = dot_nt(jnp.ones((8, blk), BF16), wa[b])
        per_ocean = 1.0 / field_o[:, 4, :]
        per_atm = 1.0 / sums_a[:, 0, :]
        sst = field_o[:, 0, :] * per_ocean
        uo = field_o[:, 1, :] * per_ocean
        vo = field_o[:, 2, :] * per_ocean
        albedo = 0.06 + 0.1 * jax.nn.sigmoid(field_o[:, 3, :] * per_ocean)
        spots = [xneed[b] >> 1 for b in range(nblocks)]
        spots = [spots[b] * owned + listed(xneed[b]) for b in range(nblocks)]

        all_of(table.at[pl.ds(0, there * owned)], push_sem.at[1]).wait()
        for b in range(nblocks):
            field_a[b] = dot_nt(table[spots[b]], wa[b])
        states = [field_a[:, f, :] * per_atm for f in range(8)]
        to_atm, to_ocn = bulk_fluxes(*states, sst, uo, vo, albedo)
        for g in range(4):
            high, low = split(to_atm[g] * wet)
            terms[:, g, :] = high
            terms[:, g + 4, :] = high
            terms[:, g + 8, :] = low
            terms[:, g + 12, :] = low
        lower = (rows >= 4).astype(jnp.int32)
        pairs = [jnp.zeros((8, blk), F32) for _ in range(npairs)]
        for b in range(nblocks):
            cells = dot_nn(terms[b].astype(BF16), wa[b])
            cells = cells[:8] + cells[8:]
            entry = xneed[b] - lower
            for index in range(npairs):
                pairs[index] = pairs[index] + jnp.where(entry == 2 * index, cells, 0.0)
        for index in range(npairs):
            back_out[index] = pairs[index]
        for index in order:
            for side in (0, 1):
                remote(
                    back_out.at[index],
                    back_in.at[index],
                    back_sem.at[0],
                    back_sem.at[1],
                    {"tile": owner(index), "sub": side},
                ).start()
        remote(back_out.at[mine], back_in.at[mine], back_sem.at[0], back_sem.at[1], {"sub": 0}).start()
        back_in[mine] = pairs[mine]

        all_of(note_in.at[pl.ds(0, there)], note_sem.at[1]).wait()
        areas = []
        places = []
        for index in range(npairs):
            note = note_out[index] if index == mine else note_in[index]
            areas.append(note[0:2])
            places.append(note[2:4])
            place[index] = jnp.concatenate(
                [jnp.broadcast_to(note[2:3], (4, blk)), jnp.broadcast_to(note[3:4], (4, blk))], 0
            )
        areas = jnp.concatenate(areas, 0)
        places = jnp.concatenate(places, 0)
        for a in range(owned):
            total = jnp.sum(jnp.where(places == float(a), areas, 0.0), 0, keepdims=True)
            inverse[a : a + 1] = 1.0 / jnp.maximum(total, 1.0)
        remote(place, place, prep_sem.at[0], prep_sem.at[1], {"sub": 0}).start()
        remote(inverse, inverse, prep_sem.at[0], prep_sem.at[1], {"sub": 0}).start()
        for g in range(5):
            high, low = split(to_ocn[g] * wet if g < 4 else wet)
            terms[:, g, :] = high
            terms[:, g + 8, :] = low
        for g in range(5, 8):
            terms[:, g, :] = jnp.zeros((nblocks, blk), F32)
            terms[:, g + 8, :] = jnp.zeros((nblocks, blk), F32)
        sums = [jnp.zeros((8, blk), F32) for _ in range(2 * half)]
        for b in range(nblocks):
            cells = dot_nn(terms[b].astype(BF16), wo[b])
            cells = cells[:8] + cells[8:]
            entry = jnp.full((8, blk), xocn[b], jnp.int32)
            for index in range(2 * half):
                sums[index] = sums[index] + jnp.where(entry == index, cells, 0.0)
        for index in range(2 * half):
            flux = sums[index][:4] / jnp.maximum(sums[index][4:5], 1.0)
            if index < half:
                shore[index] = flux
            else:
                ocn_out[index - half] = flux
        remote(shore, ocn_out, prep_sem.at[0], prep_sem.at[1], {"sub": 0}).start()

        all_of(table.at[pl.ds(0, there * owned)], push_sem.at[0]).wait()
        all_of(note_out.at[pl.ds(0, there)], note_sem.at[0]).wait()
        all_of(back_in.at[pl.ds(0, there)], back_sem.at[1]).wait()
        all_of(field_a.at[pl.ds(0, 2 * there + 1)], back_sem.at[0]).wait()
        all_of(field_a.at[pl.ds(0, 14)], prep_sem.at[0]).wait()


def landing(back, place, inverse, ocean, atm_out, ocn_out):
    npairs = back.shape[0]
    pairs = [back[index] for index in range(npairs)]
    for a in range(inverse.shape[0]):
        total = jnp.zeros(pairs[0].shape, F32)
        for index in range(npairs):
            total = total + jnp.where(place[index] == float(a), pairs[index], 0.0)
        atm_out[a] = (total[:4] + total[4:]) * inverse[a : a + 1]
    ocn_out[...] = ocean[...]


def per_device(atm_state, ocn_state, need_atm, xb_need, xb_ocn, xb_count, sea_mask, cell_area, w_atm, w_ocn):
    ntile = lax.axis_size("tile")
    fields_a = atm_state.shape[0]
    fields_o = ocn_state.shape[0]
    nblocks, blk = w_atm.shape[0], w_atm.shape[1]
    npairs = need_atm.shape[0]
    owned = atm_state.shape[1] // blk
    waters = ocn_state.shape[1] // blk
    nflux = 4
    atm = jnp.transpose(atm_state.reshape(fields_a, owned, blk), (1, 0, 2))
    ocn = jnp.transpose(ocn_state.reshape(fields_o, waters, blk), (1, 0, 2))
    dma = pltpu.SemaphoreType.DMA
    vmem = pltpu.VMEM
    in_vmem = pl.BlockSpec(memory_space=vmem)
    arrived = pl.pallas_call(
        functools.partial(kernel, ntile, npairs),
        out_shape=(
            vmem((npairs, 8, blk), F32),
            vmem((npairs, 8, blk), F32),
            vmem((owned, blk), F32),
            vmem((waters, nflux, blk), F32),
        ),
        in_specs=[pl.BlockSpec(memory_space=pl.ANY)] * 10,
        out_specs=[in_vmem] * 4,
        scratch_shapes=[
            pltpu.SMEM((2, 3, npairs), jnp.int32),
            pltpu.SMEM((2, 1), jnp.int32),
            vmem((npairs * owned, fields_a, blk), BF16),
            vmem((2 * waters, fields_o, blk), BF16),
            vmem((2 * nblocks, blk), jnp.int32),
            vmem((2 * nblocks, blk), F32),
            vmem((2 * nblocks, blk, blk), BF16),
            vmem((2 * nblocks, blk, blk), BF16),
            vmem((2 * nblocks, 8, blk), F32),
            vmem((2 * nblocks, 8, blk), F32),
            vmem((2 * nblocks, 8, blk), F32),
            vmem((2 * nblocks, 16, blk), F32),
            vmem((npairs, 4, blk), F32),
            vmem((npairs, 4, blk), F32),
            vmem((npairs, 8, blk), F32),
            vmem((waters, nflux, blk), F32),
            dma((5,)),
            dma((4,)),
            dma((4,)),
            dma((2,)),
            dma((2,)),
            dma((2,)),
            dma((2,)),
        ],
        compiler_params=pltpu.CompilerParams(
            collective_id=0, has_side_effects=True, vmem_limit_bytes=VMEM_LIMIT
        ),
    )(
        atm,
        ocn,
        need_atm,
        xb_need,
        xb_ocn,
        xb_count,
        sea_mask.reshape(nblocks, blk),
        cell_area.reshape(nblocks, blk),
        w_atm,
        w_ocn,
    )
    atm_flux, ocn_flux = pl.pallas_call(
        landing,
        out_shape=(
            jax.ShapeDtypeStruct((owned, nflux, blk), F32),
            jax.ShapeDtypeStruct((waters, nflux, blk), F32),
        ),
        in_specs=[in_vmem] * 4,
        out_specs=[in_vmem] * 2,
        compiler_params=pltpu.CompilerParams(vmem_limit_bytes=LANDING_LIMIT),
    )(*arrived)
    atm_flux = jnp.transpose(atm_flux, (1, 0, 2)).reshape(nflux, owned * blk)
    ocn_flux = jnp.transpose(ocn_flux, (1, 0, 2)).reshape(nflux, waters * blk)
    return (atm_flux, ocn_flux)


def solution(mesh):
    placed = (
        P(None, ("member", "tile")),
        P(None, ("member", "tile", "sub")),
        P(("tile", "sub")),
        P(("tile", "sub")),
        P(("tile", "sub")),
        P(("tile", "sub")),
        P(("tile", "sub")),
        P(("tile", "sub")),
        P(("tile", "sub"), None, None),
        P(("tile", "sub"), None, None),
    )
    return jax.shard_map(
        per_device,
        mesh=mesh,
        in_specs=placed,
        out_specs=(P(None, ("member", "tile")), P(None, ("member", "tile", "sub"))),
        check_vma=False,
    )
```

```python
import functools

import jax
import jax.numpy as jnp
from jax import lax
from jax.experimental import pallas as pl
from jax.experimental.pallas import tpu as pltpu
from jax.sharding import PartitionSpec as P

MESH = pl.DeviceIdType.MESH
F32 = jnp.float32
BF16 = jnp.bfloat16
VMEM_LIMIT = 60 << 20
LANDING_LIMIT = 4 << 20


def owner_offset(index, npairs, ntile):
    if index < npairs - 1:
        return index - npairs // 2 + 1
    return ntile // 2


def dot_nt(left, right):
    return lax.dot_general(left, right, (((1,), (1,)), ((), ())), preferred_element_type=F32)


def dot_nn(left, right):
    return jnp.dot(left, right, preferred_element_type=F32)


def split(value):
    high = value.astype(BF16).astype(F32)
    return high, value - high


def bulk_fluxes(ta, qa, ua, va, ps, sw, lw, pr, sst, uo, vo, albedo):
    du = ua - uo
    dv = va - vo
    factor = (0.3 + 0.1 * jnp.tanh(ps)) * jnp.sqrt(du * du + dv * dv + 1.0)
    sens = factor * (sst - ta)
    lat = factor * (0.5 * sst - qa)
    taux = factor * du
    tauy = factor * dv
    heat = (1.0 - albedo) * sw + lw - 0.2 * sst - sens - lat
    fresh = pr - 0.5 * lat
    return (sens, lat, taux, tauy), (heat, taux, tauy, fresh)


def all_of(ref, sem):
    return pltpu.make_async_copy(ref, ref, sem)


def kernel(
    ntile,
    npairs,
    atm_hbm,
    ocn_hbm,
    need_hbm,
    xneed_hbm,
    xocn_hbm,
    count_hbm,
    sea_hbm,
    area_hbm,
    wa_hbm,
    wo_hbm,
    back_in,
    place,
    inverse,
    ocn_out,
    index_s,
    count_s,
    table,
    ocean,
    sea_v,
    area_v,
    wa,
    wo,
    turned,
    field_a,
    field_o,
    sums_a,
    terms,
    note_out,
    note_in,
    back_out,
    shore,
    local_sem,
    gift_send,
    gift_recv,
    push_sem,
    note_sem,
    back_sem,
    prep_sem,
):
    tile = lax.axis_index("tile")
    core = lax.axis_index("sub")
    nblocks, blk = wa.shape[0], wa.shape[2]
    half = nblocks // 2
    owned = table.shape[0] // npairs
    mine = npairs // 2 - 1
    above = list(range(mine + 1, npairs - 1))
    below = list(range(mine))
    far_first = above[::-1] + [npairs - 1] + below
    near_first = above + [npairs - 1] + below[::-1]
    there = len(far_first)

    def asker(index):
        return lax.rem(tile + 2 * ntile - owner_offset(index, npairs, ntile), ntile)

    def owner(index):
        return lax.rem(tile + ntile + owner_offset(index, npairs, ntile), ntile)

    def remote(source, target, send, recv, where):
        return pltpu.make_async_remote_copy(
            src_ref=source, dst_ref=target, send_sem=send, recv_sem=recv, device_id=where, device_id_type=MESH
        )

    barrier = pltpu.get_barrier_semaphore()
    lists = (need_hbm, xneed_hbm, xocn_hbm)
    small = ((ocn_hbm, ocean), (sea_hbm, sea_v), (area_hbm, area_v))
    large = ((wa_hbm, wa), (wo_hbm, wo))

    def slot(ref, side):
        return ref.at[pl.ds(side * half, half)]

    @pl.when(core == 0)
    def _():
        pl.semaphore_signal(barrier, inc=1, device_id={"sub": 1}, device_id_type=MESH)
        for row, source in enumerate(lists):
            pltpu.make_async_copy(source, index_s.at[0, row], local_sem.at[1]).start()
        count = pltpu.make_async_copy(count_hbm, count_s.at[0], local_sem.at[2])
        count.start()
        pl.semaphore_wait(barrier, 1)
        for source, target in large:
            remote(source, slot(target, 0), gift_send.at[3], gift_recv.at[3], {"sub": 1}).start()
        for source, target in small:
            remote(source, slot(target, 0), gift_send.at[2], gift_recv.at[2], {"sub": 1}).start()
        all_of(index_s.at[0], local_sem.at[1]).wait()
        count.wait()
        numbers = remote(index_s.at[0], index_s.at[0], gift_send.at[0], gift_recv.at[0], {"sub": 1})
        numbers.start()
        limit = remote(count_s.at[0], count_s.at[0], gift_send.at[1], gift_recv.at[1], {"sub": 1})
        limit.start()
        numbers.wait_send()
        limit.wait_send()
        all_of(ocean, gift_send.at[2]).wait()
        all_of(wa, gift_send.at[3]).wait()
        all_of(field_a.at[pl.ds(0, 8 * 14)], prep_sem.at[1]).wait()
        all_of(back_in, back_sem.at[1]).wait()

    @pl.when(core == 1)
    def _():
        for index in far_first:
            pl.semaphore_signal(barrier, inc=1, device_id={"tile": owner(index)}, device_id_type=MESH)
        pl.semaphore_signal(barrier, inc=1, device_id={"sub": 0}, device_id_type=MESH)
        home = pltpu.make_async_copy(atm_hbm, table.at[pl.ds(mine * owned, owned)], local_sem.at[0])
        home.start()
        for row, source in enumerate(lists):
            pltpu.make_async_copy(source, index_s.at[1, row], local_sem.at[1]).start()
        count = pltpu.make_async_copy(count_hbm, count_s.at[1], local_sem.at[2])
        count.start()
        for source, target in small:
            pltpu.make_async_copy(source, slot(target, 1), local_sem.at[3]).start()
        for source, target in large:
            pltpu.make_async_copy(source, slot(target, 1), local_sem.at[4]).start()
        home.wait()
        pl.semaphore_wait(barrier, there + 1)
        for index in far_first:
            remote(
                table.at[pl.ds(mine * owned, owned)],
                table.at[pl.ds(index * owned, owned)],
                push_sem.at[0],
                push_sem.at[1],
                {"tile": asker(index)},
            ).start()
        all_of(index_s.at[1], local_sem.at[1]).wait()
        count.wait()
        all_of(ocean, local_sem.at[3]).wait()
        all_of(wa, local_sem.at[4]).wait()
        all_of(index_s.at[0], gift_recv.at[0]).wait()
        all_of(count_s.at[0], gift_recv.at[1]).wait()
        all_of(ocean, gift_recv.at[2]).wait()
        all_of(wa, gift_recv.at[3]).wait()

        def every(first, stride):
            return pl.ds(first, nblocks, stride=stride), slice(None)

        def listed(entry):
            return index_s[entry >> 3, 0, entry & 7] & (owned - 1)

        xneed = [index_s[b // half, 1, b % half] for b in range(nblocks)]
        xocn = [index_s[b // half, 2, b % half] for b in range(nblocks)]
        rows = lax.broadcasted_iota(jnp.int32, (8, blk), 0)
        block = lax.broadcasted_iota(jnp.int32, (nblocks, blk), 0)
        live = (block < jnp.where(block < half, count_s[0, 0], half + count_s[1, 0])).astype(F32)
        weighted = area_v[...] * live
        wet = weighted * sea_v[...].astype(F32)

        high, low = split(weighted)
        near = jnp.zeros((8, blk), F32)
        far = jnp.zeros((8, blk), F32)
        for b in range(nblocks):
            left = jnp.concatenate(
                [jnp.broadcast_to(high[b : b + 1], (8, blk)), jnp.broadcast_to(low[b : b + 1], (8, blk))], 0
            ).astype(BF16)
            cells = dot_nn(left, wa[b])
            cells = cells[:8] + cells[8:]
            near = near + jnp.where(rows == xneed[b], cells, 0.0)
            far = far + jnp.where(rows + 8 == xneed[b], cells, 0.0)
        for index in range(npairs):
            held = near if index < npairs // 2 else far
            at = (2 * index) % 8
            note_out[index, 0:2] = held[at : at + 2]
            for k in range(2):
                note_out[index, 2 + k : 3 + k] = jnp.full((1, blk), listed(2 * index + k), jnp.int32).astype(F32)
        for index in far_first:
            remote(
                note_out.at[index], note_in.at[index], note_sem.at[0], note_sem.at[1], {"tile": owner(index)}
            ).start()

        for b in range(nblocks):
            state = ocean[xocn[b]].astype(F32)
            left = jnp.concatenate([state, jnp.ones((8 - state.shape[0], blk), F32)], 0).astype(BF16)
            field_o[8 * b : 8 * b + 8] = dot_nt(left, wo[b])
        for b in range(nblocks):
            turned[b] = wa[b].T
            sums_a[8 * b : 8 * b + 8] = dot_nn(jnp.ones((8, blk), BF16), turned[b])
        per_ocean = 1.0 / field_o[every(4, 8)]
        per_atm = 1.0 / sums_a[every(0, 8)]
        sst = field_o[every(0, 8)] * per_ocean
        uo = field_o[every(1, 8)] * per_ocean
        vo = field_o[every(2, 8)] * per_ocean
        albedo = 0.06 + 0.1 * jax.nn.sigmoid(field_o[every(3, 8)] * per_ocean)
        spots = [xneed[b] >> 1 for b in range(nblocks)]
        spots = [spots[b] * owned + listed(xneed[b]) for b in range(nblocks)]

        all_of(table.at[pl.ds(0, there * owned)], push_sem.at[1]).wait()
        for b in range(nblocks):
            field_a[8 * b : 8 * b + 8] = dot_nn(table[spots[b]], turned[b])
        states = [field_a[every(f, 8)] * per_atm for f in range(8)]
        to_atm, to_ocn = bulk_fluxes(*states, sst, uo, vo, albedo)
        for g in range(4):
            high, low = split(to_atm[g] * wet)
            terms[every(g, 16)] = high
            terms[every(g + 4, 16)] = high
            terms[every(g + 8, 16)] = low
            terms[every(g + 12, 16)] = low
        lower = (rows >= 4).astype(jnp.int32)
        pairs = [jnp.zeros((8, blk), F32) for _ in range(npairs)]
        for b in range(nblocks):
            cells = dot_nn(terms[16 * b : 16 * b + 16].astype(BF16), wa[b])
            cells = cells[:8] + cells[8:]
            entry = xneed[b] - lower
            for index in range(npairs):
                pairs[index] = pairs[index] + jnp.where(entry == 2 * index, cells, 0.0)
        for index in range(npairs):
            back_out[index] = pairs[index]
        for index in near_first:
            for side in (0, 1):
                remote(
                    back_out.at[index],
                    back_in.at[index],
                    back_sem.at[0],
                    back_sem.at[1],
                    {"tile": owner(index), "sub": side},
                ).start()
        remote(back_out.at[mine], back_in.at[mine], back_sem.at[0], back_sem.at[1], {"sub": 0}).start()
        back_in[mine] = pairs[mine]

        all_of(note_in.at[pl.ds(0, there)], note_sem.at[1]).wait()
        areas = []
        places = []
        for index in range(npairs):
            note = note_out[index] if index == mine else note_in[index]
            areas.append(note[0:2])
            places.append(note[2:4])
            place[index] = jnp.concatenate(
                [jnp.broadcast_to(note[2:3], (4, blk)), jnp.broadcast_to(note[3:4], (4, blk))], 0
            )
        areas = jnp.concatenate(areas, 0)
        places = jnp.concatenate(places, 0)
        for a in range(owned):
            total = jnp.sum(jnp.where(places == float(a), areas, 0.0), 0, keepdims=True)
            inverse[a : a + 1] = 1.0 / jnp.maximum(total, 1.0)
        remote(place, place, prep_sem.at[0], prep_sem.at[1], {"sub": 0}).start()
        remote(inverse, inverse, prep_sem.at[0], prep_sem.at[1], {"sub": 0}).start()
        for g in range(5):
            high, low = split(to_ocn[g] * wet if g < 4 else wet)
            terms[every(g, 16)] = high
            terms[every(g + 8, 16)] = low
        for g in range(5, 8):
            terms[every(g, 16)] = jnp.zeros((nblocks, blk), F32)
            terms[every(g + 8, 16)] = jnp.zeros((nblocks, blk), F32)
        sums = [jnp.zeros((8, blk), F32) for _ in range(2 * half)]
        for b in range(nblocks):
            cells = dot_nn(terms[16 * b : 16 * b + 16].astype(BF16), wo[b])
            cells = cells[:8] + cells[8:]
            entry = jnp.full((8, blk), xocn[b], jnp.int32)
            for index in range(2 * half):
                sums[index] = sums[index] + jnp.where(entry == index, cells, 0.0)
        for index in range(2 * half):
            flux = sums[index][:4] / jnp.maximum(sums[index][4:5], 1.0)
            if index < half:
                shore[index] = flux
            else:
                ocn_out[index - half] = flux
        remote(shore, ocn_out, prep_sem.at[0], prep_sem.at[1], {"sub": 0}).start()

        all_of(table.at[pl.ds(0, there * owned)], push_sem.at[0]).wait()
        all_of(note_out.at[pl.ds(0, there)], note_sem.at[0]).wait()
        all_of(back_in.at[pl.ds(0, there)], back_sem.at[1]).wait()
        all_of(field_a.at[pl.ds(0, 8 * (2 * there + 1))], back_sem.at[0]).wait()
        all_of(field_a.at[pl.ds(0, 8 * 14)], prep_sem.at[0]).wait()


def landing(back, place, inverse, ocean, atm_out, ocn_out):
    npairs = back.shape[0]
    pairs = [back[index] for index in range(npairs)]
    for a in range(inverse.shape[0]):
        total = jnp.zeros(pairs[0].shape, F32)
        for index in range(npairs):
            total = total + jnp.where(place[index] == float(a), pairs[index], 0.0)
        atm_out[a] = (total[:4] + total[4:]) * inverse[a : a + 1]
    ocn_out[...] = ocean[...]


def per_device(atm_state, ocn_state, need_atm, xb_need, xb_ocn, xb_count, sea_mask, cell_area, w_atm, w_ocn):
    ntile = lax.axis_size("tile")
    fields_a = atm_state.shape[0]
    fields_o = ocn_state.shape[0]
    nblocks, blk = w_atm.shape[0], w_atm.shape[1]
    npairs = need_atm.shape[0]
    owned = atm_state.shape[1] // blk
    waters = ocn_state.shape[1] // blk
    nflux = 4
    atm = jnp.transpose(atm_state.reshape(fields_a, owned, blk), (1, 0, 2))
    ocn = jnp.transpose(ocn_state.reshape(fields_o, waters, blk), (1, 0, 2))
    dma = pltpu.SemaphoreType.DMA
    vmem = pltpu.VMEM
    in_vmem = pl.BlockSpec(memory_space=vmem)
    arrived = pl.pallas_call(
        functools.partial(kernel, ntile, npairs),
        out_shape=(
            vmem((npairs, 8, blk), F32),
            vmem((npairs, 8, blk), F32),
            vmem((owned, blk), F32),
            vmem((waters, nflux, blk), F32),
        ),
        in_specs=[pl.BlockSpec(memory_space=pl.ANY)] * 10,
        out_specs=[in_vmem] * 4,
        scratch_shapes=[
            pltpu.SMEM((2, 3, npairs), jnp.int32),
            pltpu.SMEM((2, 1), jnp.int32),
            vmem((npairs * owned, fields_a, blk), BF16),
            vmem((2 * waters, fields_o, blk), BF16),
            vmem((2 * nblocks, blk), jnp.int32),
            vmem((2 * nblocks, blk), F32),
            vmem((2 * nblocks, blk, blk), BF16),
            vmem((2 * nblocks, blk, blk), BF16),
            vmem((2 * nblocks, blk, blk), BF16),
            vmem((2 * nblocks * 8, blk), F32),
            vmem((2 * nblocks * 8, blk), F32),
            vmem((2 * nblocks * 8, blk), F32),
            vmem((2 * nblocks * 16, blk), F32),
            vmem((npairs, 4, blk), F32),
            vmem((npairs, 4, blk), F32),
            vmem((npairs, 8, blk), F32),
            vmem((waters, nflux, blk), F32),
            dma((5,)),
            dma((4,)),
            dma((4,)),
            dma((2,)),
            dma((2,)),
            dma((2,)),
            dma((2,)),
        ],
        compiler_params=pltpu.CompilerParams(
            collective_id=0, has_side_effects=True, vmem_limit_bytes=VMEM_LIMIT
        ),
    )(
        atm,
        ocn,
        need_atm,
        xb_need,
        xb_ocn,
        xb_count,
        sea_mask.reshape(nblocks, blk),
        cell_area.reshape(nblocks, blk),
        w_atm,
        w_ocn,
    )
    atm_flux, ocn_flux = pl.pallas_call(
        landing,
        out_shape=(
            jax.ShapeDtypeStruct((owned, nflux, blk), F32),
            jax.ShapeDtypeStruct((waters, nflux, blk), F32),
        ),
        in_specs=[in_vmem] * 4,
        out_specs=[in_vmem] * 2,
        compiler_params=pltpu.CompilerParams(vmem_limit_bytes=LANDING_LIMIT),
    )(*arrived)
    atm_flux = jnp.transpose(atm_flux, (1, 0, 2)).reshape(nflux, owned * blk)
    ocn_flux = jnp.transpose(ocn_flux, (1, 0, 2)).reshape(nflux, waters * blk)
    return (atm_flux, ocn_flux)


def solution(mesh):
    placed = (
        P(None, ("member", "tile")),
        P(None, ("member", "tile", "sub")),
        P(("tile", "sub")),
        P(("tile", "sub")),
        P(("tile", "sub")),
        P(("tile", "sub")),
        P(("tile", "sub")),
        P(("tile", "sub")),
        P(("tile", "sub"), None, None),
        P(("tile", "sub"), None, None),
    )
    return jax.shard_map(
        per_device,
        mesh=mesh,
        in_specs=placed,
        out_specs=(P(None, ("member", "tile")), P(None, ("member", "tile", "sub"))),
        check_vma=False,
    )
```

```python
import functools

import jax
import jax.numpy as jnp
from jax import lax
from jax.experimental import pallas as pl
from jax.experimental.pallas import tpu as pltpu
from jax.sharding import PartitionSpec as P

MESH = pl.DeviceIdType.MESH
F32 = jnp.float32
BF16 = jnp.bfloat16
VMEM_LIMIT = 60 << 20
LANDING_LIMIT = 4 << 20


def owner_offset(index, npairs, ntile):
    if index < npairs - 1:
        return index - npairs // 2 + 1
    return ntile // 2


def dot_nt(left, right):
    return lax.dot_general(left, right, (((1,), (1,)), ((), ())), preferred_element_type=F32)


def dot_nn(left, right):
    return jnp.dot(left, right, preferred_element_type=F32)


def split(value):
    high = value.astype(BF16).astype(F32)
    return high, value - high


def bulk_fluxes(ta, qa, ua, va, ps, sw, lw, pr, sst, uo, vo, albedo):
    du = ua - uo
    dv = va - vo
    factor = (0.3 + 0.1 * jnp.tanh(ps)) * jnp.sqrt(du * du + dv * dv + 1.0)
    sens = factor * (sst - ta)
    lat = factor * (0.5 * sst - qa)
    taux = factor * du
    tauy = factor * dv
    heat = (1.0 - albedo) * sw + lw - 0.2 * sst - sens - lat
    fresh = pr - 0.5 * lat
    return (sens, lat, taux, tauy), (heat, taux, tauy, fresh)


def all_of(ref, sem):
    return pltpu.make_async_copy(ref, ref, sem)


def kernel(
    ntile,
    npairs,
    atm_hbm,
    ocn_hbm,
    need_hbm,
    xneed_hbm,
    xocn_hbm,
    count_hbm,
    sea_hbm,
    area_hbm,
    wa_hbm,
    wo_hbm,
    back_in,
    place,
    inverse,
    ocn_out,
    index_s,
    count_s,
    first,
    second,
    ocean,
    sea_v,
    area_v,
    wa,
    wo,
    turned,
    field_a,
    field_o,
    sums_a,
    terms,
    note_out,
    note_in,
    back_out,
    shore,
    local_sem,
    gift_send,
    gift_recv,
    push_sem,
    note_sem,
    back_sem,
    prep_sem,
):
    tile = lax.axis_index("tile")
    core = lax.axis_index("sub")
    nblocks, blk = wa.shape[0], wa.shape[2]
    half = nblocks // 2
    owned = second.shape[0] // 2
    mine = npairs // 2 - 1
    above = list(range(mine + 1, npairs - 1))
    below = list(range(mine))
    top = above[-1]
    far_first = above[::-1] + [npairs - 1] + below
    near_first = above + [npairs - 1] + below[::-1]
    there = len(far_first)

    def asker(index):
        return lax.rem(tile + 2 * ntile - owner_offset(index, npairs, ntile), ntile)

    def owner(index):
        return lax.rem(tile + ntile + owner_offset(index, npairs, ntile), ntile)

    def remote(source, target, send, recv, where):
        return pltpu.make_async_remote_copy(
            src_ref=source, dst_ref=target, send_sem=send, recv_sem=recv, device_id=where, device_id_type=MESH
        )

    barrier = pltpu.get_barrier_semaphore()
    lists = (need_hbm, xneed_hbm, xocn_hbm)
    small = ((ocn_hbm, ocean), (sea_hbm, sea_v), (area_hbm, area_v))
    large = ((wa_hbm, wa), (wo_hbm, wo))

    def slot(ref, side):
        return ref.at[pl.ds(side * half, half)]

    @pl.when(core == 0)
    def _():
        pl.semaphore_signal(barrier, inc=1, device_id={"sub": 1}, device_id_type=MESH)
        home = pltpu.make_async_copy(atm_hbm, first.at[pl.ds(mine * owned, owned)], local_sem.at[0])
        home.start()
        for row, source in enumerate(lists):
            pltpu.make_async_copy(source, index_s.at[0, row], local_sem.at[1]).start()
        count = pltpu.make_async_copy(count_hbm, count_s.at[0], local_sem.at[2])
        count.start()
        for source, target in small:
            pltpu.make_async_copy(source, slot(target, 0), local_sem.at[3]).start()
        for source, target in large:
            pltpu.make_async_copy(source, slot(target, 0), local_sem.at[4]).start()
        home.wait()
        pl.semaphore_wait(barrier, 2)
        push = remote(
            first.at[pl.ds(mine * owned, owned)],
            second.at[pl.ds(0, owned)],
            push_sem.at[0],
            push_sem.at[2],
            {"tile": asker(top), "sub": 1},
        )
        push.start()
        all_of(wa, local_sem.at[4]).wait()
        for _, target in large:
            remote(slot(target, 0), slot(target, 0), gift_send.at[3], gift_recv.at[3], {"sub": 1}).start()
        all_of(ocean, local_sem.at[3]).wait()
        for _, target in small:
            remote(slot(target, 0), slot(target, 0), gift_send.at[2], gift_recv.at[2], {"sub": 1}).start()
        all_of(index_s.at[0], local_sem.at[1]).wait()
        count.wait()
        numbers = remote(index_s.at[0], index_s.at[0], gift_send.at[0], gift_recv.at[0], {"sub": 1})
        numbers.start()
        limit = remote(count_s.at[0], count_s.at[0], gift_send.at[1], gift_recv.at[1], {"sub": 1})
        limit.start()
        push.wait_send()
        numbers.wait_send()
        limit.wait_send()
        all_of(ocean, gift_send.at[2]).wait()
        all_of(wa, gift_send.at[3]).wait()
        all_of(field_a.at[pl.ds(0, 8 * 14)], prep_sem.at[1]).wait()
        all_of(back_in, back_sem.at[1]).wait()

    @pl.when(core == 1)
    def _():
        pl.semaphore_signal(barrier, inc=1, device_id={"tile": owner(top), "sub": 0}, device_id_type=MESH)
        for index in far_first:
            pl.semaphore_signal(barrier, inc=1, device_id={"tile": owner(index)}, device_id_type=MESH)
        pl.semaphore_signal(barrier, inc=1, device_id={"sub": 0}, device_id_type=MESH)
        home = pltpu.make_async_copy(atm_hbm, first.at[pl.ds(mine * owned, owned)], local_sem.at[0])
        home.start()
        for row, source in enumerate(lists):
            pltpu.make_async_copy(source, index_s.at[1, row], local_sem.at[1]).start()
        count = pltpu.make_async_copy(count_hbm, count_s.at[1], local_sem.at[2])
        count.start()
        for source, target in small:
            pltpu.make_async_copy(source, slot(target, 1), local_sem.at[3]).start()
        for source, target in large:
            pltpu.make_async_copy(source, slot(target, 1), local_sem.at[4]).start()
        home.wait()
        pl.semaphore_wait(barrier, there + 1)
        for index in far_first[1:]:
            late = index == npairs - 1
            remote(
                first.at[pl.ds(mine * owned, owned)],
                second.at[pl.ds(owned, owned)] if late else first.at[pl.ds(index * owned, owned)],
                push_sem.at[0],
                push_sem.at[2 if late else 1],
                {"tile": asker(index)},
            ).start()
        all_of(index_s.at[1], local_sem.at[1]).wait()
        count.wait()
        all_of(ocean, local_sem.at[3]).wait()
        all_of(wa, local_sem.at[4]).wait()
        all_of(index_s.at[0], gift_recv.at[0]).wait()
        all_of(count_s.at[0], gift_recv.at[1]).wait()
        all_of(ocean, gift_recv.at[2]).wait()
        all_of(wa, gift_recv.at[3]).wait()

        def every(first, stride):
            return pl.ds(first, nblocks, stride=stride), slice(None)

        def listed(entry):
            return index_s[entry >> 3, 0, entry & 7] & (owned - 1)

        xneed = [index_s[b // half, 1, b % half] for b in range(nblocks)]
        xocn = [index_s[b // half, 2, b % half] for b in range(nblocks)]
        rows = lax.broadcasted_iota(jnp.int32, (8, blk), 0)
        block = lax.broadcasted_iota(jnp.int32, (nblocks, blk), 0)
        live = (block < jnp.where(block < half, count_s[0, 0], half + count_s[1, 0])).astype(F32)
        weighted = area_v[...] * live
        wet = weighted * sea_v[...].astype(F32)

        high, low = split(weighted)
        near = jnp.zeros((8, blk), F32)
        far = jnp.zeros((8, blk), F32)
        for b in range(nblocks):
            left = jnp.concatenate(
                [jnp.broadcast_to(high[b : b + 1], (8, blk)), jnp.broadcast_to(low[b : b + 1], (8, blk))], 0
            ).astype(BF16)
            cells = dot_nn(left, wa[b])
            cells = cells[:8] + cells[8:]
            near = near + jnp.where(rows == xneed[b], cells, 0.0)
            far = far + jnp.where(rows + 8 == xneed[b], cells, 0.0)
        for index in range(npairs):
            held = near if index < npairs // 2 else far
            at = (2 * index) % 8
            note_out[index, 0:2] = held[at : at + 2]
            for k in range(2):
                note_out[index, 2 + k : 3 + k] = jnp.full((1, blk), listed(2 * index + k), jnp.int32).astype(F32)
        for index in far_first:
            remote(
                note_out.at[index], note_in.at[index], note_sem.at[0], note_sem.at[1], {"tile": owner(index)}
            ).start()

        for b in range(nblocks):
            state = ocean[xocn[b]].astype(F32)
            left = jnp.concatenate([state, jnp.ones((8 - state.shape[0], blk), F32)], 0).astype(BF16)
            field_o[8 * b : 8 * b + 8] = dot_nt(left, wo[b])
        for b in range(nblocks):
            turned[b] = wa[b].T
            sums_a[8 * b : 8 * b + 8] = dot_nn(jnp.ones((8, blk), BF16), turned[b])
        per_ocean = 1.0 / field_o[every(4, 8)]
        per_atm = 1.0 / sums_a[every(0, 8)]
        sst = field_o[every(0, 8)] * per_ocean
        uo = field_o[every(1, 8)] * per_ocean
        vo = field_o[every(2, 8)] * per_ocean
        albedo = 0.06 + 0.1 * jax.nn.sigmoid(field_o[every(3, 8)] * per_ocean)
        homes = [xneed[b] >> 1 for b in range(nblocks)]
        places = [listed(xneed[b]) for b in range(nblocks)]
        early = [jnp.minimum(homes[b], top - 1) * owned + places[b] for b in range(nblocks)]
        later = [jnp.maximum(homes[b] - top, 0) * owned + places[b] for b in range(nblocks)]
        lower = (rows >= 4).astype(jnp.int32)

        def fluxes():
            states = [field_a[every(f, 8)] * per_atm for f in range(8)]
            return bulk_fluxes(*states, sst, uo, vo, albedo)

        def send_back(to_atm, indexes):
            for g in range(4):
                high, low = split(to_atm[g] * wet)
                terms[every(g, 8)] = high
                terms[every(g + 4, 8)] = low
            pairs = {index: jnp.zeros((8, blk), F32) for index in indexes}
            for b in range(nblocks):
                cells = dot_nn(terms[8 * b : 8 * b + 8].astype(BF16), wa[b])
                cells = cells + pltpu.roll(cells, 4, 0)
                entry = xneed[b] - lower
                for index in indexes:
                    pairs[index] = pairs[index] + jnp.where(entry == 2 * index, cells, 0.0)
            for index in indexes:
                back_out[index] = pairs[index]
            for index in indexes:
                if index != mine:
                    for side in (0, 1):
                        remote(
                            back_out.at[index],
                            back_in.at[index],
                            back_sem.at[0],
                            back_sem.at[1],
                            {"tile": owner(index), "sub": side},
                        ).start()
                else:
                    remote(
                        back_out.at[mine], back_in.at[mine], back_sem.at[0], back_sem.at[1], {"sub": 0}
                    ).start()
                    back_in[mine] = pairs[mine]

        all_of(first.at[pl.ds(0, (there - 2) * owned)], push_sem.at[1]).wait()
        for b in range(nblocks):
            field_a[8 * b : 8 * b + 8] = dot_nn(first[early[b]], turned[b])
        to_atm, _ = fluxes()
        send_back(to_atm, [i for i in near_first if i < top] + [mine])
        all_of(second, push_sem.at[2]).wait()
        for b in range(nblocks):
            far_home = jnp.full((8, blk), homes[b], jnp.int32) >= top
            state = jnp.where(far_home, second[later[b]].astype(F32), first[early[b]].astype(F32)).astype(BF16)
            field_a[8 * b : 8 * b + 8] = dot_nn(state, turned[b])
        to_atm, to_ocn = fluxes()
        send_back(to_atm, [top, npairs - 1])

        all_of(note_in.at[pl.ds(0, there)], note_sem.at[1]).wait()
        areas = []
        spots = []
        for index in range(npairs):
            note = note_out[index] if index == mine else note_in[index]
            areas.append(note[0:2])
            spots.append(note[2:4])
            place[index] = jnp.concatenate(
                [jnp.broadcast_to(note[2:3], (4, blk)), jnp.broadcast_to(note[3:4], (4, blk))], 0
            )
        areas = jnp.concatenate(areas, 0)
        spots = jnp.concatenate(spots, 0)
        for a in range(owned):
            total = jnp.sum(jnp.where(spots == float(a), areas, 0.0), 0, keepdims=True)
            inverse[a : a + 1] = 1.0 / jnp.maximum(total, 1.0)
        remote(place, place, prep_sem.at[0], prep_sem.at[1], {"sub": 0}).start()
        remote(inverse, inverse, prep_sem.at[0], prep_sem.at[1], {"sub": 0}).start()
        for g in range(5):
            high, low = split(to_ocn[g] * wet if g < 4 else wet)
            terms[every(g, 16)] = high
            terms[every(g + 8, 16)] = low
        for g in range(5, 8):
            terms[every(g, 16)] = jnp.zeros((nblocks, blk), F32)
            terms[every(g + 8, 16)] = jnp.zeros((nblocks, blk), F32)
        sums = [jnp.zeros((8, blk), F32) for _ in range(2 * half)]
        for b in range(nblocks):
            cells = dot_nn(terms[16 * b : 16 * b + 16].astype(BF16), wo[b])
            cells = cells[:8] + cells[8:]
            entry = jnp.full((8, blk), xocn[b], jnp.int32)
            for index in range(2 * half):
                sums[index] = sums[index] + jnp.where(entry == index, cells, 0.0)
        for index in range(2 * half):
            flux = sums[index][:4] / jnp.maximum(sums[index][4:5], 1.0)
            if index < half:
                shore[index] = flux
            else:
                ocn_out[index - half] = flux
        remote(shore, ocn_out, prep_sem.at[0], prep_sem.at[1], {"sub": 0}).start()

        all_of(first.at[pl.ds(0, (there - 1) * owned)], push_sem.at[0]).wait()
        all_of(note_out.at[pl.ds(0, there)], note_sem.at[0]).wait()
        all_of(back_in.at[pl.ds(0, there)], back_sem.at[1]).wait()
        all_of(field_a.at[pl.ds(0, 8 * (2 * there + 1))], back_sem.at[0]).wait()
        all_of(field_a.at[pl.ds(0, 8 * 14)], prep_sem.at[0]).wait()


def landing(back, place, inverse, ocean, atm_out, ocn_out):
    npairs = back.shape[0]
    pairs = [back[index] for index in range(npairs)]
    for a in range(inverse.shape[0]):
        total = jnp.zeros(pairs[0].shape, F32)
        for index in range(npairs):
            total = total + jnp.where(place[index] == float(a), pairs[index], 0.0)
        atm_out[a] = (total[:4] + total[4:]) * inverse[a : a + 1]
    ocn_out[...] = ocean[...]


def per_device(atm_state, ocn_state, need_atm, xb_need, xb_ocn, xb_count, sea_mask, cell_area, w_atm, w_ocn):
    ntile = lax.axis_size("tile")
    fields_a = atm_state.shape[0]
    fields_o = ocn_state.shape[0]
    nblocks, blk = w_atm.shape[0], w_atm.shape[1]
    npairs = need_atm.shape[0]
    owned = atm_state.shape[1] // blk
    waters = ocn_state.shape[1] // blk
    nflux = 4
    atm = jnp.transpose(atm_state.reshape(fields_a, owned, blk), (1, 0, 2))
    ocn = jnp.transpose(ocn_state.reshape(fields_o, waters, blk), (1, 0, 2))
    dma = pltpu.SemaphoreType.DMA
    vmem = pltpu.VMEM
    in_vmem = pl.BlockSpec(memory_space=vmem)
    arrived = pl.pallas_call(
        functools.partial(kernel, ntile, npairs),
        out_shape=(
            vmem((npairs, 8, blk), F32),
            vmem((npairs, 8, blk), F32),
            vmem((owned, blk), F32),
            vmem((waters, nflux, blk), F32),
        ),
        in_specs=[pl.BlockSpec(memory_space=pl.ANY)] * 10,
        out_specs=[in_vmem] * 4,
        scratch_shapes=[
            pltpu.SMEM((2, 3, npairs), jnp.int32),
            pltpu.SMEM((2, 1), jnp.int32),
            vmem(((npairs - 2) * owned, fields_a, blk), BF16),
            vmem((2 * owned, fields_a, blk), BF16),
            vmem((2 * waters, fields_o, blk), BF16),
            vmem((2 * nblocks, blk), jnp.int32),
            vmem((2 * nblocks, blk), F32),
            vmem((2 * nblocks, blk, blk), BF16),
            vmem((2 * nblocks, blk, blk), BF16),
            vmem((2 * nblocks, blk, blk), BF16),
            vmem((2 * nblocks * 8, blk), F32),
            vmem((2 * nblocks * 8, blk), F32),
            vmem((2 * nblocks * 8, blk), F32),
            vmem((2 * nblocks * 16, blk), F32),
            vmem((npairs, 4, blk), F32),
            vmem((npairs, 4, blk), F32),
            vmem((npairs, 8, blk), F32),
            vmem((waters, nflux, blk), F32),
            dma((5,)),
            dma((4,)),
            dma((4,)),
            dma((3,)),
            dma((2,)),
            dma((2,)),
            dma((2,)),
        ],
        compiler_params=pltpu.CompilerParams(
            collective_id=0, has_side_effects=True, vmem_limit_bytes=VMEM_LIMIT
        ),
    )(
        atm,
        ocn,
        need_atm,
        xb_need,
        xb_ocn,
        xb_count,
        sea_mask.reshape(nblocks, blk),
        cell_area.reshape(nblocks, blk),
        w_atm,
        w_ocn,
    )
    atm_flux, ocn_flux = pl.pallas_call(
        landing,
        out_shape=(
            jax.ShapeDtypeStruct((owned, nflux, blk), F32),
            jax.ShapeDtypeStruct((waters, nflux, blk), F32),
        ),
        in_specs=[in_vmem] * 4,
        out_specs=[in_vmem] * 2,
        compiler_params=pltpu.CompilerParams(vmem_limit_bytes=LANDING_LIMIT),
    )(*arrived)
    atm_flux = jnp.transpose(atm_flux, (1, 0, 2)).reshape(nflux, owned * blk)
    ocn_flux = jnp.transpose(ocn_flux, (1, 0, 2)).reshape(nflux, waters * blk)
    return (atm_flux, ocn_flux)


def solution(mesh):
    placed = (
        P(None, ("member", "tile")),
        P(None, ("member", "tile", "sub")),
        P(("tile", "sub")),
        P(("tile", "sub")),
        P(("tile", "sub")),
        P(("tile", "sub")),
        P(("tile", "sub")),
        P(("tile", "sub")),
        P(("tile", "sub"), None, None),
        P(("tile", "sub"), None, None),
    )
    return jax.shard_map(
        per_device,
        mesh=mesh,
        in_specs=placed,
        out_specs=(P(None, ("member", "tile")), P(None, ("member", "tile", "sub"))),
        check_vma=False,
    )
```

```python
import functools

import jax
import jax.numpy as jnp
from jax import lax
from jax.experimental import pallas as pl
from jax.experimental.pallas import tpu as pltpu
from jax.sharding import PartitionSpec as P

MESH = pl.DeviceIdType.MESH
F32 = jnp.float32
BF16 = jnp.bfloat16
VMEM_LIMIT = 60 << 20
LANDING_LIMIT = 4 << 20


def owner_offset(index, npairs, ntile):
    if index < npairs - 1:
        return index - npairs // 2 + 1
    return ntile // 2


def dot_nt(left, right):
    return lax.dot_general(left, right, (((1,), (1,)), ((), ())), preferred_element_type=F32)


def dot_nn(left, right):
    return jnp.dot(left, right, preferred_element_type=F32)


def split(value):
    high = value.astype(BF16).astype(F32)
    return high, value - high


def bulk_fluxes(ta, qa, ua, va, ps, sw, lw, pr, sst, uo, vo, albedo):
    du = ua - uo
    dv = va - vo
    factor = (0.3 + 0.1 * jnp.tanh(ps)) * jnp.sqrt(du * du + dv * dv + 1.0)
    sens = factor * (sst - ta)
    lat = factor * (0.5 * sst - qa)
    taux = factor * du
    tauy = factor * dv
    heat = (1.0 - albedo) * sw + lw - 0.2 * sst - sens - lat
    fresh = pr - 0.5 * lat
    return (sens, lat, taux, tauy), (heat, taux, tauy, fresh)


def all_of(ref, sem):
    return pltpu.make_async_copy(ref, ref, sem)


def kernel(
    ntile,
    npairs,
    atm_hbm,
    ocn_hbm,
    need_hbm,
    xneed_hbm,
    xocn_hbm,
    count_hbm,
    sea_hbm,
    area_hbm,
    wa_hbm,
    wo_hbm,
    back_in,
    place,
    inverse,
    ocn_out,
    index_s,
    count_s,
    first,
    second,
    ocean,
    sea_v,
    area_v,
    wa,
    wo,
    turned,
    field_a,
    field_o,
    sums_a,
    terms,
    note_out,
    note_in,
    back_out,
    shore,
    local_sem,
    gift_sem,
    push_sem,
    note_sem,
    back_sem,
    prep_sem,
):
    tile = lax.axis_index("tile")
    core = lax.axis_index("sub")
    nblocks, blk = wa.shape[0], wa.shape[2]
    half = nblocks // 2
    owned = second.shape[0] // 3
    mine = npairs // 2 - 1
    above = list(range(mine + 1, npairs - 1))
    below = list(range(mine))
    top = above[-1]
    cut = top - 1
    far_first = above[::-1] + [npairs - 1] + below
    near_first = above + [npairs - 1] + below[::-1]
    there = len(far_first)

    def asker(index):
        return lax.rem(tile + 2 * ntile - owner_offset(index, npairs, ntile), ntile)

    def owner(index):
        return lax.rem(tile + ntile + owner_offset(index, npairs, ntile), ntile)

    def remote(source, target, send, recv, where):
        return pltpu.make_async_remote_copy(
            src_ref=source, dst_ref=target, send_sem=send, recv_sem=recv, device_id=where, device_id_type=MESH
        )

    barrier = pltpu.get_barrier_semaphore()
    lists = (need_hbm, xneed_hbm, xocn_hbm)
    small = ((ocn_hbm, ocean), (sea_hbm, sea_v), (area_hbm, area_v))
    large = ((wa_hbm, wa), (wo_hbm, wo))

    def slot(ref, side):
        return ref.at[pl.ds(side * half, half)]

    @pl.when(core == 0)
    def _():
        pl.semaphore_signal(barrier, inc=1, device_id={"sub": 1}, device_id_type=MESH)
        home = pltpu.make_async_copy(atm_hbm, first.at[pl.ds(mine * owned, owned)], local_sem.at[0])
        home.start()
        for row, source in enumerate(lists):
            pltpu.make_async_copy(source, index_s.at[0, row], local_sem.at[1]).start()
        count = pltpu.make_async_copy(count_hbm, count_s.at[0], local_sem.at[2])
        count.start()
        for source, target in small:
            pltpu.make_async_copy(source, slot(target, 0), local_sem.at[3]).start()
        for source, target in large:
            pltpu.make_async_copy(source, slot(target, 0), local_sem.at[4]).start()
        home.wait()
        pl.semaphore_wait(barrier, 2)
        push = remote(
            first.at[pl.ds(mine * owned, owned)],
            second.at[pl.ds(owned, owned)],
            push_sem.at[0],
            push_sem.at[2],
            {"tile": asker(top), "sub": 1},
        )
        push.start()
        all_of(wa, local_sem.at[4]).wait()
        for _, target in large:
            remote(slot(target, 0), slot(target, 0), gift_sem.at[3], gift_sem.at[3], {"sub": 1}).start()
        all_of(ocean, local_sem.at[3]).wait()
        for _, target in small:
            remote(slot(target, 0), slot(target, 0), gift_sem.at[2], gift_sem.at[2], {"sub": 1}).start()
        all_of(index_s.at[0], local_sem.at[1]).wait()
        count.wait()
        numbers = remote(index_s.at[0], index_s.at[0], gift_sem.at[0], gift_sem.at[0], {"sub": 1})
        numbers.start()
        limit = remote(count_s.at[0], count_s.at[0], gift_sem.at[1], gift_sem.at[1], {"sub": 1})
        limit.start()
        push.wait_send()
        numbers.wait_send()
        limit.wait_send()
        all_of(ocean, gift_sem.at[2]).wait()
        all_of(wa, gift_sem.at[3]).wait()
        all_of(field_a.at[pl.ds(0, 8 * 14)], prep_sem).wait()
        all_of(back_in, back_sem.at[1]).wait()

    @pl.when(core == 1)
    def _():
        pl.semaphore_signal(barrier, inc=1, device_id={"tile": owner(top), "sub": 0}, device_id_type=MESH)
        for index in near_first:
            pl.semaphore_signal(barrier, inc=1, device_id={"tile": owner(index)}, device_id_type=MESH)
        pl.semaphore_signal(barrier, inc=1, device_id={"sub": 0}, device_id_type=MESH)
        home = pltpu.make_async_copy(atm_hbm, first.at[pl.ds(mine * owned, owned)], local_sem.at[0])
        home.start()
        for row, source in enumerate(lists):
            pltpu.make_async_copy(source, index_s.at[1, row], local_sem.at[1]).start()
        count = pltpu.make_async_copy(count_hbm, count_s.at[1], local_sem.at[2])
        count.start()
        for source, target in small:
            pltpu.make_async_copy(source, slot(target, 1), local_sem.at[3]).start()
        for source, target in large:
            pltpu.make_async_copy(source, slot(target, 1), local_sem.at[4]).start()
        home.wait()
        pl.semaphore_wait(barrier, there + 1)
        for index in far_first[1:]:
            late = index >= cut
            remote(
                first.at[pl.ds(mine * owned, owned)],
                second.at[pl.ds((index - cut) * owned, owned)] if late else first.at[pl.ds(index * owned, owned)],
                push_sem.at[0],
                push_sem.at[2 if late else 1],
                {"tile": asker(index)},
            ).start()
        all_of(index_s.at[1], local_sem.at[1]).wait()
        count.wait()
        all_of(ocean, local_sem.at[3]).wait()
        all_of(wa, local_sem.at[4]).wait()
        all_of(index_s.at[0], gift_sem.at[0]).wait()
        all_of(count_s.at[0], gift_sem.at[1]).wait()
        all_of(ocean, gift_sem.at[2]).wait()
        all_of(wa, gift_sem.at[3]).wait()

        def every(first, stride):
            return pl.ds(first, nblocks, stride=stride), slice(None)

        def listed(entry):
            return index_s[entry >> 3, 0, entry & 7] & (owned - 1)

        xneed = [index_s[b // half, 1, b % half] for b in range(nblocks)]
        xocn = [index_s[b // half, 2, b % half] for b in range(nblocks)]
        rows = lax.broadcasted_iota(jnp.int32, (8, blk), 0)
        block = lax.broadcasted_iota(jnp.int32, (nblocks, blk), 0)
        live = (block < jnp.where(block < half, count_s[0, 0], half + count_s[1, 0])).astype(F32)
        weighted = area_v[...] * live
        wet = weighted * sea_v[...].astype(F32)

        high, low = split(weighted)
        near = jnp.zeros((8, blk), F32)
        far = jnp.zeros((8, blk), F32)
        for b in range(nblocks):
            left = jnp.concatenate(
                [jnp.broadcast_to(high[b : b + 1], (8, blk)), jnp.broadcast_to(low[b : b + 1], (8, blk))], 0
            ).astype(BF16)
            cells = dot_nn(left, wa[b])
            cells = cells[:8] + cells[8:]
            near = near + jnp.where(rows == xneed[b], cells, 0.0)
            far = far + jnp.where(rows + 8 == xneed[b], cells, 0.0)
        for index in range(npairs):
            held = near if index < npairs // 2 else far
            at = (2 * index) % 8
            note_out[index, 0:2] = held[at : at + 2]
            for k in range(2):
                note_out[index, 2 + k : 3 + k] = jnp.full((1, blk), listed(2 * index + k), jnp.int32).astype(F32)
        for index in far_first:
            remote(
                note_out.at[index], note_in.at[index], note_sem.at[0], note_sem.at[1], {"tile": owner(index)}
            ).start()

        for b in range(nblocks):
            state = ocean[xocn[b]].astype(F32)
            left = jnp.concatenate([state, jnp.ones((8 - state.shape[0], blk), F32)], 0).astype(BF16)
            field_o[8 * b : 8 * b + 8] = dot_nt(left, wo[b])
        for b in range(nblocks):
            turned[b] = wa[b].T
            sums_a[8 * b : 8 * b + 8] = dot_nn(jnp.ones((8, blk), BF16), turned[b])
        per_ocean = 1.0 / field_o[every(4, 8)]
        per_atm = 1.0 / sums_a[every(0, 8)]
        sst = field_o[every(0, 8)] * per_ocean
        uo = field_o[every(1, 8)] * per_ocean
        vo = field_o[every(2, 8)] * per_ocean
        albedo = 0.06 + 0.1 * jax.nn.sigmoid(field_o[every(3, 8)] * per_ocean)
        homes = [xneed[b] >> 1 for b in range(nblocks)]
        places = [listed(xneed[b]) for b in range(nblocks)]
        early = [jnp.minimum(homes[b], cut - 1) * owned + places[b] for b in range(nblocks)]
        later = [jnp.maximum(homes[b] - cut, 0) * owned + places[b] for b in range(nblocks)]
        lower = (rows >= 4).astype(jnp.int32)

        def fluxes():
            states = [field_a[every(f, 8)] * per_atm for f in range(8)]
            return bulk_fluxes(*states, sst, uo, vo, albedo)

        def send_back(to_atm, indexes):
            for g in range(4):
                high, low = split(to_atm[g] * wet)
                terms[every(g, 8)] = high
                terms[every(g + 4, 8)] = low
            pairs = {index: jnp.zeros((8, blk), F32) for index in indexes}
            for b in range(nblocks):
                cells = dot_nn(terms[8 * b : 8 * b + 8].astype(BF16), wa[b])
                cells = cells + pltpu.roll(cells, 4, 0)
                entry = xneed[b] - lower
                for index in indexes:
                    pairs[index] = pairs[index] + jnp.where(entry == 2 * index, cells, 0.0)
            for index in indexes:
                back_out[index] = pairs[index]
            for index in indexes:
                if index != mine:
                    for side in (0, 1):
                        remote(
                            back_out.at[index],
                            back_in.at[index],
                            back_sem.at[0],
                            back_sem.at[1],
                            {"tile": owner(index), "sub": side},
                        ).start()
                else:
                    remote(
                        back_out.at[mine], back_in.at[mine], back_sem.at[0], back_sem.at[1], {"sub": 0}
                    ).start()
                    back_in[mine] = pairs[mine]

        all_of(first.at[pl.ds(0, (there - 3) * owned)], push_sem.at[1]).wait()
        for b in range(nblocks):
            field_a[8 * b : 8 * b + 8] = dot_nn(first[early[b]], turned[b])
        to_atm, _ = fluxes()
        send_back(to_atm, [i for i in near_first if i < cut] + [mine])
        all_of(second, push_sem.at[2]).wait()
        for b in range(nblocks):
            far_home = jnp.full((8, blk), homes[b], jnp.int32) >= cut
            state = jnp.where(far_home, second[later[b]].astype(F32), first[early[b]].astype(F32)).astype(BF16)
            field_a[8 * b : 8 * b + 8] = dot_nn(state, turned[b])
        to_atm, to_ocn = fluxes()
        send_back(to_atm, [cut, top, npairs - 1])

        all_of(note_in.at[pl.ds(0, there)], note_sem.at[1]).wait()
        areas = []
        spots = []
        for index in range(npairs):
            note = note_out[index] if index == mine else note_in[index]
            areas.append(note[0:2])
            spots.append(note[2:4])
            place[index] = jnp.concatenate(
                [jnp.broadcast_to(note[2:3], (4, blk)), jnp.broadcast_to(note[3:4], (4, blk))], 0
            )
        areas = jnp.concatenate(areas, 0)
        spots = jnp.concatenate(spots, 0)
        for a in range(owned):
            total = jnp.sum(jnp.where(spots == float(a), areas, 0.0), 0, keepdims=True)
            inverse[a : a + 1] = 1.0 / jnp.maximum(total, 1.0)
        remote(place, place, prep_sem, prep_sem, {"sub": 0}).start()
        remote(inverse, inverse, prep_sem, prep_sem, {"sub": 0}).start()
        for g in range(5):
            high, low = split(to_ocn[g] * wet if g < 4 else wet)
            terms[every(g, 16)] = high
            terms[every(g + 8, 16)] = low
        for g in range(5, 8):
            terms[every(g, 16)] = jnp.zeros((nblocks, blk), F32)
            terms[every(g + 8, 16)] = jnp.zeros((nblocks, blk), F32)
        sums = [jnp.zeros((8, blk), F32) for _ in range(2 * half)]
        for b in range(nblocks):
            cells = dot_nn(terms[16 * b : 16 * b + 16].astype(BF16), wo[b])
            cells = cells[:8] + cells[8:]
            entry = jnp.full((8, blk), xocn[b], jnp.int32)
            for index in range(2 * half):
                sums[index] = sums[index] + jnp.where(entry == index, cells, 0.0)
        for index in range(2 * half):
            flux = sums[index][:4] / jnp.maximum(sums[index][4:5], 1.0)
            if index < half:
                shore[index] = flux
            else:
                ocn_out[index - half] = flux
        remote(shore, ocn_out, prep_sem, prep_sem, {"sub": 0}).start()

        all_of(wa.at[pl.ds(0, there - 1)], push_sem.at[0]).wait()
        all_of(note_out.at[pl.ds(0, there)], note_sem.at[0]).wait()
        all_of(back_in.at[pl.ds(0, there)], back_sem.at[1]).wait()
        all_of(field_a.at[pl.ds(0, 8 * (2 * there + 1))], back_sem.at[0]).wait()
        all_of(field_a.at[pl.ds(0, 8 * 14)], prep_sem).wait()


def landing(back, place, inverse, ocean, atm_out, ocn_out):
    npairs = back.shape[0]
    pairs = [back[index] for index in range(npairs)]
    for a in range(inverse.shape[0]):
        total = jnp.zeros(pairs[0].shape, F32)
        for index in range(npairs):
            total = total + jnp.where(place[index] == float(a), pairs[index], 0.0)
        atm_out[a] = (total[:4] + total[4:]) * inverse[a : a + 1]
    ocn_out[...] = ocean[...]


def per_device(atm_state, ocn_state, need_atm, xb_need, xb_ocn, xb_count, sea_mask, cell_area, w_atm, w_ocn):
    ntile = lax.axis_size("tile")
    fields_a = atm_state.shape[0]
    fields_o = ocn_state.shape[0]
    nblocks, blk = w_atm.shape[0], w_atm.shape[1]
    npairs = need_atm.shape[0]
    owned = atm_state.shape[1] // blk
    waters = ocn_state.shape[1] // blk
    nflux = 4
    atm = jnp.transpose(atm_state.reshape(fields_a, owned, blk), (1, 0, 2))
    ocn = jnp.transpose(ocn_state.reshape(fields_o, waters, blk), (1, 0, 2))
    dma = pltpu.SemaphoreType.DMA
    vmem = pltpu.VMEM
    in_vmem = pl.BlockSpec(memory_space=vmem)
    arrived = pl.pallas_call(
        functools.partial(kernel, ntile, npairs),
        out_shape=(
            vmem((npairs, 8, blk), F32),
            vmem((npairs, 8, blk), F32),
            vmem((owned, blk), F32),
            vmem((waters, nflux, blk), F32),
        ),
        in_specs=[pl.BlockSpec(memory_space=pl.ANY)] * 10,
        out_specs=[in_vmem] * 4,
        scratch_shapes=[
            pltpu.SMEM((2, 3, npairs), jnp.int32),
            pltpu.SMEM((2, 1), jnp.int32),
            vmem(((npairs - 3) * owned, fields_a, blk), BF16),
            vmem((3 * owned, fields_a, blk), BF16),
            vmem((2 * waters, fields_o, blk), BF16),
            vmem((2 * nblocks, blk), jnp.int32),
            vmem((2 * nblocks, blk), F32),
            vmem((2 * nblocks, blk, blk), BF16),
            vmem((2 * nblocks, blk, blk), BF16),
            vmem((2 * nblocks, blk, blk), BF16),
            vmem((2 * nblocks * 8, blk), F32),
            vmem((2 * nblocks * 8, blk), F32),
            vmem((2 * nblocks * 8, blk), F32),
            vmem((2 * nblocks * 16, blk), F32),
            vmem((npairs, 4, blk), F32),
            vmem((npairs, 4, blk), F32),
            vmem((npairs, 8, blk), F32),
            vmem((waters, nflux, blk), F32),
            dma((5,)),
            dma((4,)),
            dma((3,)),
            dma((2,)),
            dma((2,)),
            dma,
        ],
        compiler_params=pltpu.CompilerParams(
            collective_id=0, has_side_effects=True, vmem_limit_bytes=VMEM_LIMIT
        ),
    )(
        atm,
        ocn,
        need_atm,
        xb_need,
        xb_ocn,
        xb_count,
        sea_mask.reshape(nblocks, blk),
        cell_area.reshape(nblocks, blk),
        w_atm,
        w_ocn,
    )
    atm_flux, ocn_flux = pl.pallas_call(
        landing,
        out_shape=(
            jax.ShapeDtypeStruct((owned, nflux, blk), F32),
            jax.ShapeDtypeStruct((waters, nflux, blk), F32),
        ),
        in_specs=[in_vmem] * 4,
        out_specs=[in_vmem] * 2,
        compiler_params=pltpu.CompilerParams(vmem_limit_bytes=LANDING_LIMIT),
    )(*arrived)
    atm_flux = jnp.transpose(atm_flux, (1, 0, 2)).reshape(nflux, owned * blk)
    ocn_flux = jnp.transpose(ocn_flux, (1, 0, 2)).reshape(nflux, waters * blk)
    return (atm_flux, ocn_flux)


def solution(mesh):
    placed = (
        P(None, ("member", "tile")),
        P(None, ("member", "tile", "sub")),
        P(("tile", "sub")),
        P(("tile", "sub")),
        P(("tile", "sub")),
        P(("tile", "sub")),
        P(("tile", "sub")),
        P(("tile", "sub")),
        P(("tile", "sub"), None, None),
        P(("tile", "sub"), None, None),
    )
    return jax.shard_map(
        per_device,
        mesh=mesh,
        in_specs=placed,
        out_specs=(P(None, ("member", "tile")), P(None, ("member", "tile", "sub"))),
        check_vma=False,
    )
```

```python
import functools

import jax
import jax.numpy as jnp
from jax import lax
from jax.experimental import pallas as pl
from jax.experimental.pallas import tpu as pltpu
from jax.sharding import PartitionSpec as P

MESH = pl.DeviceIdType.MESH
F32 = jnp.float32
BF16 = jnp.bfloat16
VMEM_LIMIT = 60 << 20
LANDING_LIMIT = 4 << 20


def owner_offset(index, npairs, ntile):
    if index < npairs - 1:
        return index - npairs // 2 + 1
    return ntile // 2


def dot_nt(left, right):
    return lax.dot_general(left, right, (((1,), (1,)), ((), ())), preferred_element_type=F32)


def dot_nn(left, right):
    return jnp.dot(left, right, preferred_element_type=F32)


def split(value):
    high = value.astype(BF16).astype(F32)
    return high, value - high


def bulk_fluxes(ta, qa, ua, va, ps, sw, lw, pr, sst, uo, vo, albedo):
    du = ua - uo
    dv = va - vo
    factor = (0.3 + 0.1 * jnp.tanh(ps)) * jnp.sqrt(du * du + dv * dv + 1.0)
    sens = factor * (sst - ta)
    lat = factor * (0.5 * sst - qa)
    taux = factor * du
    tauy = factor * dv
    heat = (1.0 - albedo) * sw + lw - 0.2 * sst - sens - lat
    fresh = pr - 0.5 * lat
    return (sens, lat, taux, tauy), (heat, taux, tauy, fresh)


def all_of(ref, sem):
    return pltpu.make_async_copy(ref, ref, sem)


def kernel(
    ntile,
    npairs,
    atm_hbm,
    ocn_hbm,
    need_hbm,
    xneed_hbm,
    xocn_hbm,
    count_hbm,
    sea_hbm,
    area_hbm,
    wa_hbm,
    wo_hbm,
    back_in,
    place,
    inverse,
    ocn_out,
    index_s,
    count_s,
    first,
    second,
    ocean,
    sea_v,
    area_v,
    wa,
    wo,
    turned,
    field_a,
    field_o,
    sums_a,
    terms,
    note_out,
    note_in,
    back_out,
    shore,
    local_sem,
    gift_sem,
    push_sem,
    note_sem,
    back_sem,
    prep_sem,
):
    tile = lax.axis_index("tile")
    core = lax.axis_index("sub")
    nblocks, blk = wa.shape[0], wa.shape[2]
    half = nblocks // 2
    owned = second.shape[0] // 3
    mine = npairs // 2 - 1
    above = list(range(mine + 1, npairs - 1))
    below = list(range(mine))
    top = above[-1]
    cut = top - 1
    far_first = above[::-1] + [npairs - 1] + below
    near_first = above + [npairs - 1] + below[::-1]
    there = len(far_first)

    def asker(index):
        return lax.rem(tile + 2 * ntile - owner_offset(index, npairs, ntile), ntile)

    def owner(index):
        return lax.rem(tile + ntile + owner_offset(index, npairs, ntile), ntile)

    def remote(source, target, send, recv, where):
        return pltpu.make_async_remote_copy(
            src_ref=source, dst_ref=target, send_sem=send, recv_sem=recv, device_id=where, device_id_type=MESH
        )

    barrier = pltpu.get_barrier_semaphore()
    lists = (need_hbm, xneed_hbm, xocn_hbm)
    small = ((ocn_hbm, ocean), (sea_hbm, sea_v), (area_hbm, area_v))
    large = ((wa_hbm, wa), (wo_hbm, wo))

    def slot(ref, side):
        return ref.at[pl.ds(side * half, half)]

    @pl.when(core == 0)
    def _():
        pl.semaphore_signal(barrier, inc=1, device_id={"sub": 1}, device_id_type=MESH)
        home = pltpu.make_async_copy(atm_hbm, first.at[pl.ds(mine * owned, owned)], local_sem.at[0])
        home.start()
        for row, source in enumerate(lists):
            pltpu.make_async_copy(source, index_s.at[0, row], local_sem.at[1]).start()
        count = pltpu.make_async_copy(count_hbm, count_s.at[0], local_sem.at[2])
        count.start()
        for source, target in small:
            pltpu.make_async_copy(source, slot(target, 0), local_sem.at[3]).start()
        for source, target in large:
            pltpu.make_async_copy(source, slot(target, 0), local_sem.at[4]).start()
        home.wait()
        pl.semaphore_wait(barrier, 3)
        for index in (top, npairs - 1):
            remote(
                first.at[pl.ds(mine * owned, owned)],
                second.at[pl.ds((index - cut) * owned, owned)],
                push_sem.at[0],
                push_sem.at[2],
                {"tile": asker(index), "sub": 1},
            ).start()
        all_of(wa, local_sem.at[4]).wait()
        for _, target in large:
            remote(slot(target, 0), slot(target, 0), gift_sem.at[3], gift_sem.at[3], {"sub": 1}).start()
        all_of(ocean, local_sem.at[3]).wait()
        for _, target in small:
            remote(slot(target, 0), slot(target, 0), gift_sem.at[2], gift_sem.at[2], {"sub": 1}).start()
        all_of(index_s.at[0], local_sem.at[1]).wait()
        count.wait()
        numbers = remote(index_s.at[0], index_s.at[0], gift_sem.at[0], gift_sem.at[0], {"sub": 1})
        numbers.start()
        limit = remote(count_s.at[0], count_s.at[0], gift_sem.at[1], gift_sem.at[1], {"sub": 1})
        limit.start()
        all_of(first.at[pl.ds(0, 2 * owned)], push_sem.at[0]).wait()
        numbers.wait_send()
        limit.wait_send()
        all_of(ocean, gift_sem.at[2]).wait()
        all_of(wa, gift_sem.at[3]).wait()
        all_of(field_a.at[pl.ds(0, 8 * 14)], prep_sem).wait()
        all_of(back_in, back_sem.at[1]).wait()

    @pl.when(core == 1)
    def _():
        pl.semaphore_signal(barrier, inc=1, device_id={"tile": owner(top), "sub": 0}, device_id_type=MESH)
        for index in near_first:
            side = 0 if index == npairs - 1 else 1
            pl.semaphore_signal(
                barrier, inc=1, device_id={"tile": owner(index), "sub": side}, device_id_type=MESH
            )
        pl.semaphore_signal(barrier, inc=1, device_id={"sub": 0}, device_id_type=MESH)
        home = pltpu.make_async_copy(atm_hbm, first.at[pl.ds(mine * owned, owned)], local_sem.at[0])
        home.start()
        for row, source in enumerate(lists):
            pltpu.make_async_copy(source, index_s.at[1, row], local_sem.at[1]).start()
        count = pltpu.make_async_copy(count_hbm, count_s.at[1], local_sem.at[2])
        count.start()
        for source, target in small:
            pltpu.make_async_copy(source, slot(target, 1), local_sem.at[3]).start()
        for source, target in large:
            pltpu.make_async_copy(source, slot(target, 1), local_sem.at[4]).start()
        home.wait()
        pl.semaphore_wait(barrier, there)
        for index in [i for i in far_first[1:] if i != npairs - 1]:
            late = index >= cut
            remote(
                first.at[pl.ds(mine * owned, owned)],
                second.at[pl.ds((index - cut) * owned, owned)] if late else first.at[pl.ds(index * owned, owned)],
                push_sem.at[0],
                push_sem.at[2 if late else 1],
                {"tile": asker(index)},
            ).start()
        all_of(index_s.at[1], local_sem.at[1]).wait()
        count.wait()
        all_of(ocean, local_sem.at[3]).wait()
        all_of(wa, local_sem.at[4]).wait()
        all_of(index_s.at[0], gift_sem.at[0]).wait()
        all_of(count_s.at[0], gift_sem.at[1]).wait()
        all_of(ocean, gift_sem.at[2]).wait()
        all_of(wa, gift_sem.at[3]).wait()

        def every(first, stride):
            return pl.ds(first, nblocks, stride=stride), slice(None)

        def listed(entry):
            return index_s[entry >> 3, 0, entry & 7] & (owned - 1)

        xneed = [index_s[b // half, 1, b % half] for b in range(nblocks)]
        xocn = [index_s[b // half, 2, b % half] for b in range(nblocks)]
        rows = lax.broadcasted_iota(jnp.int32, (8, blk), 0)
        block = lax.broadcasted_iota(jnp.int32, (nblocks, blk), 0)
        live = (block < jnp.where(block < half, count_s[0, 0], half + count_s[1, 0])).astype(F32)
        weighted = area_v[...] * live
        wet = weighted * sea_v[...].astype(F32)

        high, low = split(weighted)
        near = jnp.zeros((8, blk), F32)
        far = jnp.zeros((8, blk), F32)
        for b in range(nblocks):
            left = jnp.concatenate(
                [jnp.broadcast_to(high[b : b + 1], (8, blk)), jnp.broadcast_to(low[b : b + 1], (8, blk))], 0
            ).astype(BF16)
            cells = dot_nn(left, wa[b])
            cells = cells[:8] + cells[8:]
            near = near + jnp.where(rows == xneed[b], cells, 0.0)
            far = far + jnp.where(rows + 8 == xneed[b], cells, 0.0)
        for index in range(npairs):
            held = near if index < npairs // 2 else far
            at = (2 * index) % 8
            note_out[index, 0:2] = held[at : at + 2]
            for k in range(2):
                note_out[index, 2 + k : 3 + k] = jnp.full((1, blk), listed(2 * index + k), jnp.int32).astype(F32)

        def send_note(index):
            remote(
                note_out.at[index], note_in.at[index], note_sem.at[0], note_sem.at[1], {"tile": owner(index)}
            ).start()

        for index in far_first:
            if index != npairs - 1:
                send_note(index)

        for b in range(nblocks):
            state = ocean[xocn[b]].astype(F32)
            left = jnp.concatenate([state, jnp.ones((8 - state.shape[0], blk), F32)], 0).astype(BF16)
            field_o[8 * b : 8 * b + 8] = dot_nt(left, wo[b])
        for b in range(nblocks):
            turned[b] = wa[b].T
            sums_a[8 * b : 8 * b + 8] = dot_nn(jnp.ones((8, blk), BF16), turned[b])
        per_ocean = 1.0 / field_o[every(4, 8)]
        per_atm = 1.0 / sums_a[every(0, 8)]
        sst = field_o[every(0, 8)] * per_ocean
        uo = field_o[every(1, 8)] * per_ocean
        vo = field_o[every(2, 8)] * per_ocean
        albedo = 0.06 + 0.1 * jax.nn.sigmoid(field_o[every(3, 8)] * per_ocean)
        homes = [xneed[b] >> 1 for b in range(nblocks)]
        places = [listed(xneed[b]) for b in range(nblocks)]
        early = [jnp.minimum(homes[b], cut - 1) * owned + places[b] for b in range(nblocks)]
        later = [jnp.maximum(homes[b] - cut, 0) * owned + places[b] for b in range(nblocks)]
        lower = (rows >= 4).astype(jnp.int32)

        def fluxes():
            states = [field_a[every(f, 8)] * per_atm for f in range(8)]
            return bulk_fluxes(*states, sst, uo, vo, albedo)

        def send_back(to_atm, indexes):
            for g in range(4):
                high, low = split(to_atm[g] * wet)
                terms[every(g, 8)] = high
                terms[every(g + 4, 8)] = low
            pairs = {index: jnp.zeros((8, blk), F32) for index in indexes}
            for b in range(nblocks):
                cells = dot_nn(terms[8 * b : 8 * b + 8].astype(BF16), wa[b])
                cells = cells + pltpu.roll(cells, 4, 0)
                entry = xneed[b] - lower
                for index in indexes:
                    pairs[index] = pairs[index] + jnp.where(entry == 2 * index, cells, 0.0)
            for index in indexes:
                back_out[index] = pairs[index]
            for index in indexes:
                if index != mine:
                    for side in (0, 1):
                        remote(
                            back_out.at[index],
                            back_in.at[index],
                            back_sem.at[0],
                            back_sem.at[1],
                            {"tile": owner(index), "sub": side},
                        ).start()
                else:
                    remote(
                        back_out.at[mine], back_in.at[mine], back_sem.at[0], back_sem.at[1], {"sub": 0}
                    ).start()
                    back_in[mine] = pairs[mine]

        all_of(first.at[pl.ds(0, (there - 3) * owned)], push_sem.at[1]).wait()
        for b in range(nblocks):
            field_a[8 * b : 8 * b + 8] = dot_nn(first[early[b]], turned[b])
        to_atm, _ = fluxes()
        send_back(to_atm, [i for i in near_first if i < cut] + [mine])
        all_of(second, push_sem.at[2]).wait()
        send_note(npairs - 1)
        for b in range(nblocks):
            far_home = jnp.full((8, blk), homes[b], jnp.int32) >= cut
            state = jnp.where(far_home, second[later[b]].astype(F32), first[early[b]].astype(F32)).astype(BF16)
            field_a[8 * b : 8 * b + 8] = dot_nn(state, turned[b])
        to_atm, to_ocn = fluxes()
        send_back(to_atm, [cut, top, npairs - 1])

        all_of(note_in.at[pl.ds(0, there)], note_sem.at[1]).wait()
        areas = []
        spots = []
        for index in range(npairs):
            note = note_out[index] if index == mine else note_in[index]
            areas.append(note[0:2])
            spots.append(note[2:4])
            place[index] = jnp.concatenate(
                [jnp.broadcast_to(note[2:3], (4, blk)), jnp.broadcast_to(note[3:4], (4, blk))], 0
            )
        areas = jnp.concatenate(areas, 0)
        spots = jnp.concatenate(spots, 0)
        for a in range(owned):
            total = jnp.sum(jnp.where(spots == float(a), areas, 0.0), 0, keepdims=True)
            inverse[a : a + 1] = 1.0 / jnp.maximum(total, 1.0)
        remote(place, place, prep_sem, prep_sem, {"sub": 0}).start()
        remote(inverse, inverse, prep_sem, prep_sem, {"sub": 0}).start()
        for g in range(5):
            high, low = split(to_ocn[g] * wet if g < 4 else wet)
            terms[every(g, 16)] = high
            terms[every(g + 8, 16)] = low
        for g in range(5, 8):
            terms[every(g, 16)] = jnp.zeros((nblocks, blk), F32)
            terms[every(g + 8, 16)] = jnp.zeros((nblocks, blk), F32)
        sums = [jnp.zeros((8, blk), F32) for _ in range(2 * half)]
        for b in range(nblocks):
            cells = dot_nn(terms[16 * b : 16 * b + 16].astype(BF16), wo[b])
            cells = cells[:8] + cells[8:]
            entry = jnp.full((8, blk), xocn[b], jnp.int32)
            for index in range(2 * half):
                sums[index] = sums[index] + jnp.where(entry == index, cells, 0.0)
        for index in range(2 * half):
            flux = sums[index][:4] / jnp.maximum(sums[index][4:5], 1.0)
            if index < half:
                shore[index] = flux
            else:
                ocn_out[index - half] = flux
        remote(shore, ocn_out, prep_sem, prep_sem, {"sub": 0}).start()

        all_of(wa.at[pl.ds(0, there - 2)], push_sem.at[0]).wait()
        all_of(note_out.at[pl.ds(0, there)], note_sem.at[0]).wait()
        all_of(back_in.at[pl.ds(0, there)], back_sem.at[1]).wait()
        all_of(field_a.at[pl.ds(0, 8 * (2 * there + 1))], back_sem.at[0]).wait()
        all_of(field_a.at[pl.ds(0, 8 * 14)], prep_sem).wait()


def landing(back, place, inverse, ocean, atm_out, ocn_out):
    npairs = back.shape[0]
    pairs = [back[index] for index in range(npairs)]
    for a in range(inverse.shape[0]):
        total = jnp.zeros(pairs[0].shape, F32)
        for index in range(npairs):
            total = total + jnp.where(place[index] == float(a), pairs[index], 0.0)
        atm_out[a] = (total[:4] + total[4:]) * inverse[a : a + 1]
    ocn_out[...] = ocean[...]


def per_device(atm_state, ocn_state, need_atm, xb_need, xb_ocn, xb_count, sea_mask, cell_area, w_atm, w_ocn):
    ntile = lax.axis_size("tile")
    fields_a = atm_state.shape[0]
    fields_o = ocn_state.shape[0]
    nblocks, blk = w_atm.shape[0], w_atm.shape[1]
    npairs = need_atm.shape[0]
    owned = atm_state.shape[1] // blk
    waters = ocn_state.shape[1] // blk
    nflux = 4
    atm = jnp.transpose(atm_state.reshape(fields_a, owned, blk), (1, 0, 2))
    ocn = jnp.transpose(ocn_state.reshape(fields_o, waters, blk), (1, 0, 2))
    dma = pltpu.SemaphoreType.DMA
    vmem = pltpu.VMEM
    in_vmem = pl.BlockSpec(memory_space=vmem)
    arrived = pl.pallas_call(
        functools.partial(kernel, ntile, npairs),
        out_shape=(
            vmem((npairs, 8, blk), F32),
            vmem((npairs, 8, blk), F32),
            vmem((owned, blk), F32),
            vmem((waters, nflux, blk), F32),
        ),
        in_specs=[pl.BlockSpec(memory_space=pl.ANY)] * 10,
        out_specs=[in_vmem] * 4,
        scratch_shapes=[
            pltpu.SMEM((2, 3, npairs), jnp.int32),
            pltpu.SMEM((2, 1), jnp.int32),
            vmem(((npairs - 3) * owned, fields_a, blk), BF16),
            vmem((3 * owned, fields_a, blk), BF16),
            vmem((2 * waters, fields_o, blk), BF16),
            vmem((2 * nblocks, blk), jnp.int32),
            vmem((2 * nblocks, blk), F32),
            vmem((2 * nblocks, blk, blk), BF16),
            vmem((2 * nblocks, blk, blk), BF16),
            vmem((2 * nblocks, blk, blk), BF16),
            vmem((2 * nblocks * 8, blk), F32),
            vmem((2 * nblocks * 8, blk), F32),
            vmem((2 * nblocks * 8, blk), F32),
            vmem((2 * nblocks * 16, blk), F32),
            vmem((npairs, 4, blk), F32),
            vmem((npairs, 4, blk), F32),
            vmem((npairs, 8, blk), F32),
            vmem((waters, nflux, blk), F32),
            dma((5,)),
            dma((4,)),
            dma((3,)),
            dma((2,)),
            dma((2,)),
            dma,
        ],
        compiler_params=pltpu.CompilerParams(
            collective_id=0, has_side_effects=True, vmem_limit_bytes=VMEM_LIMIT
        ),
    )(
        atm,
        ocn,
        need_atm,
        xb_need,
        xb_ocn,
        xb_count,
        sea_mask.reshape(nblocks, blk),
        cell_area.reshape(nblocks, blk),
        w_atm,
        w_ocn,
    )
    atm_flux, ocn_flux = pl.pallas_call(
        landing,
        out_shape=(
            jax.ShapeDtypeStruct((owned, nflux, blk), F32),
            jax.ShapeDtypeStruct((waters, nflux, blk), F32),
        ),
        in_specs=[in_vmem] * 4,
        out_specs=[in_vmem] * 2,
        compiler_params=pltpu.CompilerParams(vmem_limit_bytes=LANDING_LIMIT),
    )(*arrived)
    atm_flux = jnp.transpose(atm_flux, (1, 0, 2)).reshape(nflux, owned * blk)
    ocn_flux = jnp.transpose(ocn_flux, (1, 0, 2)).reshape(nflux, waters * blk)
    return (atm_flux, ocn_flux)


def solution(mesh):
    placed = (
        P(None, ("member", "tile")),
        P(None, ("member", "tile", "sub")),
        P(("tile", "sub")),
        P(("tile", "sub")),
        P(("tile", "sub")),
        P(("tile", "sub")),
        P(("tile", "sub")),
        P(("tile", "sub")),
        P(("tile", "sub"), None, None),
        P(("tile", "sub"), None, None),
    )
    return jax.shard_map(
        per_device,
        mesh=mesh,
        in_specs=placed,
        out_specs=(P(None, ("member", "tile")), P(None, ("member", "tile", "sub"))),
        check_vma=False,
    )
```

```python
import functools

import jax
import jax.numpy as jnp
from jax import lax
from jax.experimental import pallas as pl
from jax.experimental.pallas import tpu as pltpu
from jax.sharding import PartitionSpec as P

MESH = pl.DeviceIdType.MESH
F32 = jnp.float32
BF16 = jnp.bfloat16
VMEM_LIMIT = 60 << 20
LANDING_LIMIT = 4 << 20


def owner_offset(index, npairs, ntile):
    if index < npairs - 1:
        return index - npairs // 2 + 1
    return ntile // 2


def dot_nt(left, right):
    return lax.dot_general(left, right, (((1,), (1,)), ((), ())), preferred_element_type=F32)


def dot_nn(left, right):
    return jnp.dot(left, right, preferred_element_type=F32)


def split(value):
    high = value.astype(BF16).astype(F32)
    return high, value - high


def bulk_fluxes(ta, qa, ua, va, ps, sw, lw, pr, sst, uo, vo, albedo):
    du = ua - uo
    dv = va - vo
    factor = (0.3 + 0.1 * jnp.tanh(ps)) * jnp.sqrt(du * du + dv * dv + 1.0)
    sens = factor * (sst - ta)
    lat = factor * (0.5 * sst - qa)
    taux = factor * du
    tauy = factor * dv
    heat = (1.0 - albedo) * sw + lw - 0.2 * sst - sens - lat
    fresh = pr - 0.5 * lat
    return (sens, lat, taux, tauy), (heat, taux, tauy, fresh)


def all_of(ref, sem):
    return pltpu.make_async_copy(ref, ref, sem)


def kernel(
    ntile,
    npairs,
    atm_hbm,
    ocn_hbm,
    need_hbm,
    xneed_hbm,
    xocn_hbm,
    count_hbm,
    sea_hbm,
    area_hbm,
    wa_hbm,
    wo_hbm,
    back_in,
    place,
    inverse,
    ocn_out,
    index_s,
    count_s,
    first,
    second,
    ocean,
    sea_v,
    area_v,
    wa,
    wo,
    turned,
    field_a,
    field_o,
    sums_a,
    terms,
    note_out,
    note_in,
    back_out,
    shore,
    local_sem,
    gift_sem,
    push_sem,
    note_sem,
    back_sem,
    prep_sem,
):
    tile = lax.axis_index("tile")
    core = lax.axis_index("sub")
    nblocks, blk = wa.shape[0], wa.shape[2]
    half = nblocks // 2
    owned = second.shape[0] // 3
    mine = npairs // 2 - 1
    above = list(range(mine + 1, npairs - 1))
    below = list(range(mine))
    top = above[-1]
    cut = top - 1
    far_first = above[::-1] + [npairs - 1] + below
    near_first = above + [npairs - 1] + below[::-1]
    there = len(far_first)

    def asker(index):
        return lax.rem(tile + 2 * ntile - owner_offset(index, npairs, ntile), ntile)

    def owner(index):
        return lax.rem(tile + ntile + owner_offset(index, npairs, ntile), ntile)

    def remote(source, target, send, recv, where):
        return pltpu.make_async_remote_copy(
            src_ref=source, dst_ref=target, send_sem=send, recv_sem=recv, device_id=where, device_id_type=MESH
        )

    barrier = pltpu.get_barrier_semaphore()
    lists = (need_hbm, xneed_hbm, xocn_hbm)
    small = ((ocn_hbm, ocean), (sea_hbm, sea_v), (area_hbm, area_v))
    large = ((wa_hbm, wa), (wo_hbm, wo))

    def slot(ref, side):
        return ref.at[pl.ds(side * half, half)]

    @pl.when(core == 0)
    def _():
        pl.semaphore_signal(barrier, inc=1, device_id={"sub": 1}, device_id_type=MESH)
        home = pltpu.make_async_copy(atm_hbm, first.at[pl.ds(mine * owned, owned)], local_sem.at[0])
        home.start()
        for row, source in enumerate(lists):
            pltpu.make_async_copy(source, index_s.at[0, row], local_sem.at[1]).start()
        count = pltpu.make_async_copy(count_hbm, count_s.at[0], local_sem.at[2])
        count.start()
        for source, target in small:
            pltpu.make_async_copy(source, slot(target, 0), local_sem.at[3]).start()
        for source, target in large:
            pltpu.make_async_copy(source, slot(target, 0), local_sem.at[4]).start()
        home.wait()
        pl.semaphore_wait(barrier, 3)
        for index in (top, npairs - 1):
            remote(
                first.at[pl.ds(mine * owned, owned)],
                second.at[pl.ds((index - cut) * owned, owned)],
                push_sem.at[0],
                push_sem.at[2],
                {"tile": asker(index), "sub": 1},
            ).start()
        all_of(wa, local_sem.at[4]).wait()
        for _, target in large:
            remote(slot(target, 0), slot(target, 0), gift_sem.at[3], gift_sem.at[3], {"sub": 1}).start()
        all_of(ocean, local_sem.at[3]).wait()
        for _, target in small:
            remote(slot(target, 0), slot(target, 0), gift_sem.at[2], gift_sem.at[2], {"sub": 1}).start()
        all_of(index_s.at[0], local_sem.at[1]).wait()
        count.wait()
        numbers = remote(index_s.at[0], index_s.at[0], gift_sem.at[0], gift_sem.at[0], {"sub": 1})
        numbers.start()
        limit = remote(count_s.at[0], count_s.at[0], gift_sem.at[1], gift_sem.at[1], {"sub": 1})
        limit.start()
        all_of(first.at[pl.ds(0, 2 * owned)], push_sem.at[0]).wait()
        numbers.wait_send()
        limit.wait_send()
        all_of(ocean, gift_sem.at[2]).wait()
        all_of(wa, gift_sem.at[3]).wait()
        all_of(field_a.at[pl.ds(0, 8 * 14)], prep_sem).wait()
        all_of(back_in, back_sem.at[1]).wait()

    @pl.when(core == 1)
    def _():
        pl.semaphore_signal(barrier, inc=1, device_id={"tile": owner(top), "sub": 0}, device_id_type=MESH)
        for index in near_first:
            side = 0 if index == npairs - 1 else 1
            pl.semaphore_signal(
                barrier, inc=1, device_id={"tile": owner(index), "sub": side}, device_id_type=MESH
            )
        pl.semaphore_signal(barrier, inc=1, device_id={"sub": 0}, device_id_type=MESH)
        home = pltpu.make_async_copy(atm_hbm, first.at[pl.ds(mine * owned, owned)], local_sem.at[0])
        home.start()
        for row, source in enumerate(lists):
            pltpu.make_async_copy(source, index_s.at[1, row], local_sem.at[1]).start()
        count = pltpu.make_async_copy(count_hbm, count_s.at[1], local_sem.at[2])
        count.start()
        for source, target in small:
            pltpu.make_async_copy(source, slot(target, 1), local_sem.at[3]).start()
        for source, target in large:
            pltpu.make_async_copy(source, slot(target, 1), local_sem.at[4]).start()
        home.wait()
        pl.semaphore_wait(barrier, there)
        for index in [i for i in far_first[1:] if i != npairs - 1]:
            late = index >= cut
            remote(
                first.at[pl.ds(mine * owned, owned)],
                second.at[pl.ds((index - cut) * owned, owned)] if late else first.at[pl.ds(index * owned, owned)],
                push_sem.at[0],
                push_sem.at[2 if late else 1],
                {"tile": asker(index)},
            ).start()
        all_of(index_s.at[1], local_sem.at[1]).wait()
        count.wait()
        all_of(ocean, local_sem.at[3]).wait()
        all_of(wa, local_sem.at[4]).wait()

        def turn(blocks):
            for b in blocks:
                turned[b] = wa[b].T
                sums_a[8 * b : 8 * b + 8] = dot_nn(jnp.ones((8, blk), BF16), turned[b])

        turn(range(half, nblocks))
        all_of(index_s.at[0], gift_sem.at[0]).wait()
        all_of(count_s.at[0], gift_sem.at[1]).wait()
        all_of(ocean, gift_sem.at[2]).wait()
        all_of(wa, gift_sem.at[3]).wait()

        def every(first, stride):
            return pl.ds(first, nblocks, stride=stride), slice(None)

        def listed(entry):
            return index_s[entry >> 3, 0, entry & 7] & (owned - 1)

        xneed = [index_s[b // half, 1, b % half] for b in range(nblocks)]
        xocn = [index_s[b // half, 2, b % half] for b in range(nblocks)]
        rows = lax.broadcasted_iota(jnp.int32, (8, blk), 0)
        block = lax.broadcasted_iota(jnp.int32, (nblocks, blk), 0)
        live = (block < jnp.where(block < half, count_s[0, 0], half + count_s[1, 0])).astype(F32)
        weighted = area_v[...] * live
        wet = weighted * sea_v[...].astype(F32)

        high, low = split(weighted)
        near = jnp.zeros((8, blk), F32)
        far = jnp.zeros((8, blk), F32)
        for b in range(nblocks):
            left = jnp.concatenate(
                [jnp.broadcast_to(high[b : b + 1], (8, blk)), jnp.broadcast_to(low[b : b + 1], (8, blk))], 0
            ).astype(BF16)
            cells = dot_nn(left, wa[b])
            cells = cells[:8] + cells[8:]
            near = near + jnp.where(rows == xneed[b], cells, 0.0)
            far = far + jnp.where(rows + 8 == xneed[b], cells, 0.0)
        for index in range(npairs):
            held = near if index < npairs // 2 else far
            at = (2 * index) % 8
            note_out[index, 0:2] = held[at : at + 2]
            for k in range(2):
                note_out[index, 2 + k : 3 + k] = jnp.full((1, blk), listed(2 * index + k), jnp.int32).astype(F32)

        def send_note(index):
            remote(
                note_out.at[index], note_in.at[index], note_sem.at[0], note_sem.at[1], {"tile": owner(index)}
            ).start()

        for index in far_first:
            if index != npairs - 1:
                send_note(index)

        for b in range(nblocks):
            state = ocean[xocn[b]].astype(F32)
            left = jnp.concatenate([state, jnp.ones((8 - state.shape[0], blk), F32)], 0).astype(BF16)
            field_o[8 * b : 8 * b + 8] = dot_nt(left, wo[b])
        turn(range(half))
        per_ocean = 1.0 / field_o[every(4, 8)]
        per_atm = 1.0 / sums_a[every(0, 8)]
        sst = field_o[every(0, 8)] * per_ocean
        uo = field_o[every(1, 8)] * per_ocean
        vo = field_o[every(2, 8)] * per_ocean
        albedo = 0.06 + 0.1 * jax.nn.sigmoid(field_o[every(3, 8)] * per_ocean)
        homes = [xneed[b] >> 1 for b in range(nblocks)]
        places = [listed(xneed[b]) for b in range(nblocks)]
        early = [jnp.minimum(homes[b], cut - 1) * owned + places[b] for b in range(nblocks)]
        later = [jnp.maximum(homes[b] - cut, 0) * owned + places[b] for b in range(nblocks)]
        lower = (rows >= 4).astype(jnp.int32)

        def fluxes():
            states = [field_a[every(f, 8)] * per_atm for f in range(8)]
            return bulk_fluxes(*states, sst, uo, vo, albedo)

        def send_back(to_atm, indexes):
            for g in range(4):
                high, low = split(to_atm[g] * wet)
                terms[every(g, 8)] = high
                terms[every(g + 4, 8)] = low
            pairs = {index: jnp.zeros((8, blk), F32) for index in indexes}
            for b in range(nblocks):
                cells = dot_nn(terms[8 * b : 8 * b + 8].astype(BF16), wa[b])
                cells = cells + pltpu.roll(cells, 4, 0)
                entry = xneed[b] - lower
                for index in indexes:
                    pairs[index] = pairs[index] + jnp.where(entry == 2 * index, cells, 0.0)
            for index in indexes:
                back_out[index] = pairs[index]
            for index in indexes:
                if index != mine:
                    for side in (0, 1):
                        remote(
                            back_out.at[index],
                            back_in.at[index],
                            back_sem.at[0],
                            back_sem.at[1],
                            {"tile": owner(index), "sub": side},
                        ).start()
                else:
                    remote(
                        back_out.at[mine], back_in.at[mine], back_sem.at[0], back_sem.at[1], {"sub": 0}
                    ).start()
                    back_in[mine] = pairs[mine]

        all_of(first.at[pl.ds(0, (there - 3) * owned)], push_sem.at[1]).wait()
        for b in range(nblocks):
            field_a[8 * b : 8 * b + 8] = dot_nn(first[early[b]], turned[b])
        to_atm, _ = fluxes()
        send_back(to_atm, [i for i in near_first if i < cut] + [mine])
        all_of(second, push_sem.at[2]).wait()
        send_note(npairs - 1)
        for b in range(nblocks):
            far_home = jnp.full((8, blk), homes[b], jnp.int32) >= cut
            state = jnp.where(far_home, second[later[b]].astype(F32), first[early[b]].astype(F32)).astype(BF16)
            field_a[8 * b : 8 * b + 8] = dot_nn(state, turned[b])
        to_atm, to_ocn = fluxes()
        send_back(to_atm, [cut, top, npairs - 1])

        all_of(note_in.at[pl.ds(0, there)], note_sem.at[1]).wait()
        areas = []
        spots = []
        for index in range(npairs):
            note = note_out[index] if index == mine else note_in[index]
            areas.append(note[0:2])
            spots.append(note[2:4])
            place[index] = jnp.concatenate(
                [jnp.broadcast_to(note[2:3], (4, blk)), jnp.broadcast_to(note[3:4], (4, blk))], 0
            )
        areas = jnp.concatenate(areas, 0)
        spots = jnp.concatenate(spots, 0)
        for a in range(owned):
            total = jnp.sum(jnp.where(spots == float(a), areas, 0.0), 0, keepdims=True)
            inverse[a : a + 1] = 1.0 / jnp.maximum(total, 1.0)
        remote(place, place, prep_sem, prep_sem, {"sub": 0}).start()
        remote(inverse, inverse, prep_sem, prep_sem, {"sub": 0}).start()
        for g in range(5):
            high, low = split(to_ocn[g] * wet if g < 4 else wet)
            terms[every(g, 16)] = high
            terms[every(g + 8, 16)] = low
        for g in range(5, 8):
            terms[every(g, 16)] = jnp.zeros((nblocks, blk), F32)
            terms[every(g + 8, 16)] = jnp.zeros((nblocks, blk), F32)
        sums = [jnp.zeros((8, blk), F32) for _ in range(2 * half)]
        for b in range(nblocks):
            cells = dot_nn(terms[16 * b : 16 * b + 16].astype(BF16), wo[b])
            cells = cells[:8] + cells[8:]
            entry = jnp.full((8, blk), xocn[b], jnp.int32)
            for index in range(2 * half):
                sums[index] = sums[index] + jnp.where(entry == index, cells, 0.0)
        for index in range(2 * half):
            flux = sums[index][:4] / jnp.maximum(sums[index][4:5], 1.0)
            if index < half:
                shore[index] = flux
            else:
                ocn_out[index - half] = flux
        remote(shore, ocn_out, prep_sem, prep_sem, {"sub": 0}).start()

        all_of(wa.at[pl.ds(0, there - 2)], push_sem.at[0]).wait()
        all_of(note_out.at[pl.ds(0, there)], note_sem.at[0]).wait()
        all_of(back_in.at[pl.ds(0, there)], back_sem.at[1]).wait()
        all_of(field_a.at[pl.ds(0, 8 * (2 * there + 1))], back_sem.at[0]).wait()
        all_of(field_a.at[pl.ds(0, 8 * 14)], prep_sem).wait()


def landing(back, place, inverse, ocean, atm_out, ocn_out):
    npairs = back.shape[0]
    pairs = [back[index] for index in range(npairs)]
    for a in range(inverse.shape[0]):
        total = jnp.zeros(pairs[0].shape, F32)
        for index in range(npairs):
            total = total + jnp.where(place[index] == float(a), pairs[index], 0.0)
        atm_out[a] = (total[:4] + total[4:]) * inverse[a : a + 1]
    ocn_out[...] = ocean[...]


def per_device(atm_state, ocn_state, need_atm, xb_need, xb_ocn, xb_count, sea_mask, cell_area, w_atm, w_ocn):
    ntile = lax.axis_size("tile")
    fields_a = atm_state.shape[0]
    fields_o = ocn_state.shape[0]
    nblocks, blk = w_atm.shape[0], w_atm.shape[1]
    npairs = need_atm.shape[0]
    owned = atm_state.shape[1] // blk
    waters = ocn_state.shape[1] // blk
    nflux = 4
    atm = jnp.transpose(atm_state.reshape(fields_a, owned, blk), (1, 0, 2))
    ocn = jnp.transpose(ocn_state.reshape(fields_o, waters, blk), (1, 0, 2))
    dma = pltpu.SemaphoreType.DMA
    vmem = pltpu.VMEM
    in_vmem = pl.BlockSpec(memory_space=vmem)
    arrived = pl.pallas_call(
        functools.partial(kernel, ntile, npairs),
        out_shape=(
            vmem((npairs, 8, blk), F32),
            vmem((npairs, 8, blk), F32),
            vmem((owned, blk), F32),
            vmem((waters, nflux, blk), F32),
        ),
        in_specs=[pl.BlockSpec(memory_space=pl.ANY)] * 10,
        out_specs=[in_vmem] * 4,
        scratch_shapes=[
            pltpu.SMEM((2, 3, npairs), jnp.int32),
            pltpu.SMEM((2, 1), jnp.int32),
            vmem(((npairs - 3) * owned, fields_a, blk), BF16),
            vmem((3 * owned, fields_a, blk), BF16),
            vmem((2 * waters, fields_o, blk), BF16),
            vmem((2 * nblocks, blk), jnp.int32),
            vmem((2 * nblocks, blk), F32),
            vmem((2 * nblocks, blk, blk), BF16),
            vmem((2 * nblocks, blk, blk), BF16),
            vmem((2 * nblocks, blk, blk), BF16),
            vmem((2 * nblocks * 8, blk), F32),
            vmem((2 * nblocks * 8, blk), F32),
            vmem((2 * nblocks * 8, blk), F32),
            vmem((2 * nblocks * 16, blk), F32),
            vmem((npairs, 4, blk), F32),
            vmem((npairs, 4, blk), F32),
            vmem((npairs, 8, blk), F32),
            vmem((waters, nflux, blk), F32),
            dma((5,)),
            dma((4,)),
            dma((3,)),
            dma((2,)),
            dma((2,)),
            dma,
        ],
        compiler_params=pltpu.CompilerParams(
            collective_id=0, has_side_effects=True, vmem_limit_bytes=VMEM_LIMIT
        ),
    )(
        atm,
        ocn,
        need_atm,
        xb_need,
        xb_ocn,
        xb_count,
        sea_mask.reshape(nblocks, blk),
        cell_area.reshape(nblocks, blk),
        w_atm,
        w_ocn,
    )
    atm_flux, ocn_flux = pl.pallas_call(
        landing,
        out_shape=(
            jax.ShapeDtypeStruct((owned, nflux, blk), F32),
            jax.ShapeDtypeStruct((waters, nflux, blk), F32),
        ),
        in_specs=[in_vmem] * 4,
        out_specs=[in_vmem] * 2,
        compiler_params=pltpu.CompilerParams(vmem_limit_bytes=LANDING_LIMIT),
    )(*arrived)
    atm_flux = jnp.transpose(atm_flux, (1, 0, 2)).reshape(nflux, owned * blk)
    ocn_flux = jnp.transpose(ocn_flux, (1, 0, 2)).reshape(nflux, waters * blk)
    return (atm_flux, ocn_flux)


def solution(mesh):
    placed = (
        P(None, ("member", "tile")),
        P(None, ("member", "tile", "sub")),
        P(("tile", "sub")),
        P(("tile", "sub")),
        P(("tile", "sub")),
        P(("tile", "sub")),
        P(("tile", "sub")),
        P(("tile", "sub")),
        P(("tile", "sub"), None, None),
        P(("tile", "sub"), None, None),
    )
    return jax.shard_map(
        per_device,
        mesh=mesh,
        in_specs=placed,
        out_specs=(P(None, ("member", "tile")), P(None, ("member", "tile", "sub"))),
        check_vma=False,
    )
```

```python
import functools

import jax
import jax.numpy as jnp
from jax import lax
from jax.experimental import pallas as pl
from jax.experimental.pallas import tpu as pltpu
from jax.sharding import PartitionSpec as P

MESH = pl.DeviceIdType.MESH
F32 = jnp.float32
BF16 = jnp.bfloat16
VMEM_LIMIT = 60 << 20
LANDING_LIMIT = 4 << 20


def owner_offset(index, npairs, ntile):
    if index < npairs - 1:
        return index - npairs // 2 + 1
    return ntile // 2


def dot_nt(left, right):
    return lax.dot_general(left, right, (((1,), (1,)), ((), ())), preferred_element_type=F32)


def dot_nn(left, right):
    return jnp.dot(left, right, preferred_element_type=F32)


def split(value):
    high = value.astype(BF16).astype(F32)
    return high, value - high


def bulk_fluxes(ta, qa, ua, va, ps, sw, lw, pr, sst, uo, vo, albedo):
    du = ua - uo
    dv = va - vo
    factor = (0.3 + 0.1 * jnp.tanh(ps)) * jnp.sqrt(du * du + dv * dv + 1.0)
    sens = factor * (sst - ta)
    lat = factor * (0.5 * sst - qa)
    taux = factor * du
    tauy = factor * dv
    heat = (1.0 - albedo) * sw + lw - 0.2 * sst - sens - lat
    fresh = pr - 0.5 * lat
    return (sens, lat, taux, tauy), (heat, taux, tauy, fresh)


def all_of(ref, sem):
    return pltpu.make_async_copy(ref, ref, sem)


def kernel(
    ntile,
    npairs,
    atm_hbm,
    ocn_hbm,
    need_hbm,
    xneed_hbm,
    xocn_hbm,
    count_hbm,
    sea_hbm,
    area_hbm,
    wa_hbm,
    wo_hbm,
    back_in,
    place,
    inverse,
    ocn_out,
    index_s,
    count_s,
    first,
    second,
    ocean,
    sea_v,
    area_v,
    wa,
    wo,
    turned,
    field_a,
    field_o,
    sums_a,
    terms,
    note_out,
    note_in,
    back_out,
    shore,
    local_sem,
    gift_sem,
    push_sem,
    note_sem,
    back_sem,
    prep_sem,
):
    tile = lax.axis_index("tile")
    core = lax.axis_index("sub")
    nblocks, blk = wa.shape[0], wa.shape[2]
    half = nblocks // 2
    owned = second.shape[0] // 3
    mine = npairs // 2 - 1
    above = list(range(mine + 1, npairs - 1))
    below = list(range(mine))
    top = above[-1]
    cut = top - 1
    far_first = above[::-1] + [npairs - 1] + below
    near_first = above + [npairs - 1] + below[::-1]
    there = len(far_first)

    def asker(index):
        return lax.rem(tile + 2 * ntile - owner_offset(index, npairs, ntile), ntile)

    def owner(index):
        return lax.rem(tile + ntile + owner_offset(index, npairs, ntile), ntile)

    def remote(source, target, send, recv, where):
        return pltpu.make_async_remote_copy(
            src_ref=source, dst_ref=target, send_sem=send, recv_sem=recv, device_id=where, device_id_type=MESH
        )

    barrier = pltpu.get_barrier_semaphore()
    lists = (need_hbm, xneed_hbm, xocn_hbm)
    small = ((ocn_hbm, ocean), (sea_hbm, sea_v), (area_hbm, area_v))
    large = ((wa_hbm, wa), (wo_hbm, wo))

    def slot(ref, side):
        return ref.at[pl.ds(side * half, half)]

    @pl.when(core == 0)
    def _():
        pl.semaphore_signal(barrier, inc=1, device_id={"sub": 1}, device_id_type=MESH)
        home = pltpu.make_async_copy(atm_hbm, first.at[pl.ds(mine * owned, owned)], local_sem.at[0])
        home.start()
        for row, source in enumerate(lists):
            pltpu.make_async_copy(source, index_s.at[0, row], local_sem.at[1]).start()
        count = pltpu.make_async_copy(count_hbm, count_s.at[0], local_sem.at[2])
        count.start()
        for source, target in small:
            pltpu.make_async_copy(source, slot(target, 0), local_sem.at[3]).start()
        for source, target in large:
            pltpu.make_async_copy(source, slot(target, 0), local_sem.at[4]).start()
        home.wait()
        pl.semaphore_wait(barrier, 3)
        for index in (top, npairs - 1):
            remote(
                first.at[pl.ds(mine * owned, owned)],
                second.at[pl.ds((index - cut) * owned, owned)],
                push_sem.at[0],
                push_sem.at[2],
                {"tile": asker(index), "sub": 1},
            ).start()
        all_of(wa, local_sem.at[4]).wait()
        for _, target in large:
            remote(slot(target, 0), slot(target, 0), gift_sem.at[3], gift_sem.at[3], {"sub": 1}).start()
        all_of(ocean, local_sem.at[3]).wait()
        for _, target in small:
            remote(slot(target, 0), slot(target, 0), gift_sem.at[2], gift_sem.at[2], {"sub": 1}).start()
        all_of(index_s.at[0], local_sem.at[1]).wait()
        count.wait()
        numbers = remote(index_s.at[0], index_s.at[0], gift_sem.at[0], gift_sem.at[0], {"sub": 1})
        numbers.start()
        limit = remote(count_s.at[0], count_s.at[0], gift_sem.at[1], gift_sem.at[1], {"sub": 1})
        limit.start()
        all_of(first.at[pl.ds(0, 2 * owned)], push_sem.at[0]).wait()
        numbers.wait_send()
        limit.wait_send()
        all_of(ocean, gift_sem.at[2]).wait()
        all_of(wa, gift_sem.at[3]).wait()
        all_of(field_a.at[pl.ds(0, 8 * 14)], prep_sem).wait()
        all_of(back_in, back_sem.at[1]).wait()

    @pl.when(core == 1)
    def _():
        pl.semaphore_signal(barrier, inc=1, device_id={"tile": owner(top), "sub": 0}, device_id_type=MESH)
        for index in [npairs - 1] + [i for i in near_first if i != npairs - 1]:
            side = 0 if index == npairs - 1 else 1
            pl.semaphore_signal(
                barrier, inc=1, device_id={"tile": owner(index), "sub": side}, device_id_type=MESH
            )
        pl.semaphore_signal(barrier, inc=1, device_id={"sub": 0}, device_id_type=MESH)
        home = pltpu.make_async_copy(atm_hbm, first.at[pl.ds(mine * owned, owned)], local_sem.at[0])
        home.start()
        for row, source in enumerate(lists):
            pltpu.make_async_copy(source, index_s.at[1, row], local_sem.at[1]).start()
        count = pltpu.make_async_copy(count_hbm, count_s.at[1], local_sem.at[2])
        count.start()
        for source, target in small:
            pltpu.make_async_copy(source, slot(target, 1), local_sem.at[3]).start()
        for source, target in large:
            pltpu.make_async_copy(source, slot(target, 1), local_sem.at[4]).start()
        home.wait()
        pl.semaphore_wait(barrier, there)
        for index in [i for i in far_first[1:] if i != npairs - 1]:
            late = index >= cut
            remote(
                first.at[pl.ds(mine * owned, owned)],
                second.at[pl.ds((index - cut) * owned, owned)] if late else first.at[pl.ds(index * owned, owned)],
                push_sem.at[0],
                push_sem.at[2 if late else 1],
                {"tile": asker(index)},
            ).start()
        all_of(index_s.at[1], local_sem.at[1]).wait()
        count.wait()
        all_of(ocean, local_sem.at[3]).wait()
        all_of(wa, local_sem.at[4]).wait()
        all_of(index_s.at[0], gift_sem.at[0]).wait()
        all_of(count_s.at[0], gift_sem.at[1]).wait()
        all_of(ocean, gift_sem.at[2]).wait()
        all_of(wa, gift_sem.at[3]).wait()

        def every(first, stride):
            return pl.ds(first, nblocks, stride=stride), slice(None)

        def listed(entry):
            return index_s[entry >> 3, 0, entry & 7] & (owned - 1)

        xneed = [index_s[b // half, 1, b % half] for b in range(nblocks)]
        xocn = [index_s[b // half, 2, b % half] for b in range(nblocks)]
        rows = lax.broadcasted_iota(jnp.int32, (8, blk), 0)
        block = lax.broadcasted_iota(jnp.int32, (nblocks, blk), 0)
        live = (block < jnp.where(block < half, count_s[0, 0], half + count_s[1, 0])).astype(F32)
        weighted = area_v[...] * live
        wet = weighted * sea_v[...].astype(F32)

        high, low = split(weighted)
        near = jnp.zeros((8, blk), F32)
        far = jnp.zeros((8, blk), F32)
        for b in range(nblocks):
            left = jnp.concatenate(
                [jnp.broadcast_to(high[b : b + 1], (8, blk)), jnp.broadcast_to(low[b : b + 1], (8, blk))], 0
            ).astype(BF16)
            cells = dot_nn(left, wa[b])
            cells = cells[:8] + cells[8:]
            near = near + jnp.where(rows == xneed[b], cells, 0.0)
            far = far + jnp.where(rows + 8 == xneed[b], cells, 0.0)
        for index in range(npairs):
            held = near if index < npairs // 2 else far
            at = (2 * index) % 8
            note_out[index, 0:2] = held[at : at + 2]
            for k in range(2):
                note_out[index, 2 + k : 3 + k] = jnp.full((1, blk), listed(2 * index + k), jnp.int32).astype(F32)

        def send_note(index):
            remote(
                note_out.at[index], note_in.at[index], note_sem.at[0], note_sem.at[1], {"tile": owner(index)}
            ).start()

        for index in far_first:
            if index != npairs - 1:
                send_note(index)

        for b in range(nblocks):
            state = ocean[xocn[b]].astype(F32)
            left = jnp.concatenate([state, jnp.ones((8 - state.shape[0], blk), F32)], 0).astype(BF16)
            field_o[8 * b : 8 * b + 8] = dot_nt(left, wo[b])
        for b in range(nblocks):
            turned[b] = wa[b].T
            sums_a[8 * b : 8 * b + 8] = dot_nn(jnp.ones((8, blk), BF16), turned[b])
        per_ocean = 1.0 / field_o[every(4, 8)]
        per_atm = 1.0 / sums_a[every(0, 8)]
        sst = field_o[every(0, 8)] * per_ocean
        uo = field_o[every(1, 8)] * per_ocean
        vo = field_o[every(2, 8)] * per_ocean
        albedo = 0.06 + 0.1 * jax.nn.sigmoid(field_o[every(3, 8)] * per_ocean)
        homes = [xneed[b] >> 1 for b in range(nblocks)]
        places = [listed(xneed[b]) for b in range(nblocks)]
        early = [jnp.minimum(homes[b], cut - 1) * owned + places[b] for b in range(nblocks)]
        later = [jnp.maximum(homes[b] - cut, 0) * owned + places[b] for b in range(nblocks)]
        lower = (rows >= 4).astype(jnp.int32)

        def fluxes():
            states = [field_a[every(f, 8)] * per_atm for f in range(8)]
            return bulk_fluxes(*states, sst, uo, vo, albedo)

        def send_back(to_atm, indexes):
            for g in range(4):
                high, low = split(to_atm[g] * wet)
                terms[every(g, 8)] = high
                terms[every(g + 4, 8)] = low
            pairs = {index: jnp.zeros((8, blk), F32) for index in indexes}
            for b in range(nblocks):
                cells = dot_nn(terms[8 * b : 8 * b + 8].astype(BF16), wa[b])
                cells = cells + pltpu.roll(cells, 4, 0)
                entry = xneed[b] - lower
                for index in indexes:
                    pairs[index] = pairs[index] + jnp.where(entry == 2 * index, cells, 0.0)
            for index in indexes:
                back_out[index] = pairs[index]
            for index in indexes:
                if index != mine:
                    for side in (0, 1):
                        remote(
                            back_out.at[index],
                            back_in.at[index],
                            back_sem.at[0],
                            back_sem.at[1],
                            {"tile": owner(index), "sub": side},
                        ).start()
                else:
                    remote(
                        back_out.at[mine], back_in.at[mine], back_sem.at[0], back_sem.at[1], {"sub": 0}
                    ).start()
                    back_in[mine] = pairs[mine]

        all_of(first.at[pl.ds(0, (there - 3) * owned)], push_sem.at[1]).wait()
        for b in range(nblocks):
            field_a[8 * b : 8 * b + 8] = dot_nn(first[early[b]], turned[b])
        to_atm, _ = fluxes()
        send_back(to_atm, [i for i in near_first if i < cut] + [mine])
        all_of(second, push_sem.at[2]).wait()
        send_note(npairs - 1)
        for b in range(nblocks):
            far_home = jnp.full((8, blk), homes[b], jnp.int32) >= cut
            state = jnp.where(far_home, second[later[b]].astype(F32), first[early[b]].astype(F32)).astype(BF16)
            field_a[8 * b : 8 * b + 8] = dot_nn(state, turned[b])
        to_atm, to_ocn = fluxes()
        send_back(to_atm, [cut, top, npairs - 1])

        all_of(note_in.at[pl.ds(0, there)], note_sem.at[1]).wait()
        areas = []
        spots = []
        for index in range(npairs):
            note = note_out[index] if index == mine else note_in[index]
            areas.append(note[0:2])
            spots.append(note[2:4])
            place[index] = jnp.concatenate(
                [jnp.broadcast_to(note[2:3], (4, blk)), jnp.broadcast_to(note[3:4], (4, blk))], 0
            )
        areas = jnp.concatenate(areas, 0)
        spots = jnp.concatenate(spots, 0)
        for a in range(owned):
            total = jnp.sum(jnp.where(spots == float(a), areas, 0.0), 0, keepdims=True)
            inverse[a : a + 1] = 1.0 / jnp.maximum(total, 1.0)
        remote(place, place, prep_sem, prep_sem, {"sub": 0}).start()
        remote(inverse, inverse, prep_sem, prep_sem, {"sub": 0}).start()
        for g in range(5):
            high, low = split(to_ocn[g] * wet if g < 4 else wet)
            terms[every(g, 16)] = high
            terms[every(g + 8, 16)] = low
        for g in range(5, 8):
            terms[every(g, 16)] = jnp.zeros((nblocks, blk), F32)
            terms[every(g + 8, 16)] = jnp.zeros((nblocks, blk), F32)
        sums = [jnp.zeros((8, blk), F32) for _ in range(2 * half)]
        for b in range(nblocks):
            cells = dot_nn(terms[16 * b : 16 * b + 16].astype(BF16), wo[b])
            cells = cells[:8] + cells[8:]
            entry = jnp.full((8, blk), xocn[b], jnp.int32)
            for index in range(2 * half):
                sums[index] = sums[index] + jnp.where(entry == index, cells, 0.0)
        for index in range(2 * half):
            flux = sums[index][:4] / jnp.maximum(sums[index][4:5], 1.0)
            if index < half:
                shore[index] = flux
            else:
                ocn_out[index - half] = flux
        remote(shore, ocn_out, prep_sem, prep_sem, {"sub": 0}).start()

        all_of(wa.at[pl.ds(0, there - 2)], push_sem.at[0]).wait()
        all_of(note_out.at[pl.ds(0, there)], note_sem.at[0]).wait()
        all_of(back_in.at[pl.ds(0, there)], back_sem.at[1]).wait()
        all_of(field_a.at[pl.ds(0, 8 * (2 * there + 1))], back_sem.at[0]).wait()
        all_of(field_a.at[pl.ds(0, 8 * 14)], prep_sem).wait()


def landing(back, place, inverse, ocean, atm_out, ocn_out):
    npairs = back.shape[0]
    pairs = [back[index] for index in range(npairs)]
    for a in range(inverse.shape[0]):
        total = jnp.zeros(pairs[0].shape, F32)
        for index in range(npairs):
            total = total + jnp.where(place[index] == float(a), pairs[index], 0.0)
        atm_out[a] = (total[:4] + total[4:]) * inverse[a : a + 1]
    ocn_out[...] = ocean[...]


def per_device(atm_state, ocn_state, need_atm, xb_need, xb_ocn, xb_count, sea_mask, cell_area, w_atm, w_ocn):
    ntile = lax.axis_size("tile")
    fields_a = atm_state.shape[0]
    fields_o = ocn_state.shape[0]
    nblocks, blk = w_atm.shape[0], w_atm.shape[1]
    npairs = need_atm.shape[0]
    owned = atm_state.shape[1] // blk
    waters = ocn_state.shape[1] // blk
    nflux = 4
    atm = jnp.transpose(atm_state.reshape(fields_a, owned, blk), (1, 0, 2))
    ocn = jnp.transpose(ocn_state.reshape(fields_o, waters, blk), (1, 0, 2))
    dma = pltpu.SemaphoreType.DMA
    vmem = pltpu.VMEM
    in_vmem = pl.BlockSpec(memory_space=vmem)
    arrived = pl.pallas_call(
        functools.partial(kernel, ntile, npairs),
        out_shape=(
            vmem((npairs, 8, blk), F32),
            vmem((npairs, 8, blk), F32),
            vmem((owned, blk), F32),
            vmem((waters, nflux, blk), F32),
        ),
        in_specs=[pl.BlockSpec(memory_space=pl.ANY)] * 10,
        out_specs=[in_vmem] * 4,
        scratch_shapes=[
            pltpu.SMEM((2, 3, npairs), jnp.int32),
            pltpu.SMEM((2, 1), jnp.int32),
            vmem(((npairs - 3) * owned, fields_a, blk), BF16),
            vmem((3 * owned, fields_a, blk), BF16),
            vmem((2 * waters, fields_o, blk), BF16),
            vmem((2 * nblocks, blk), jnp.int32),
            vmem((2 * nblocks, blk), F32),
            vmem((2 * nblocks, blk, blk), BF16),
            vmem((2 * nblocks, blk, blk), BF16),
            vmem((2 * nblocks, blk, blk), BF16),
            vmem((2 * nblocks * 8, blk), F32),
            vmem((2 * nblocks * 8, blk), F32),
            vmem((2 * nblocks * 8, blk), F32),
            vmem((2 * nblocks * 16, blk), F32),
            vmem((npairs, 4, blk), F32),
            vmem((npairs, 4, blk), F32),
            vmem((npairs, 8, blk), F32),
            vmem((waters, nflux, blk), F32),
            dma((5,)),
            dma((4,)),
            dma((3,)),
            dma((2,)),
            dma((2,)),
            dma,
        ],
        compiler_params=pltpu.CompilerParams(
            collective_id=0, has_side_effects=True, vmem_limit_bytes=VMEM_LIMIT
        ),
    )(
        atm,
        ocn,
        need_atm,
        xb_need,
        xb_ocn,
        xb_count,
        sea_mask.reshape(nblocks, blk),
        cell_area.reshape(nblocks, blk),
        w_atm,
        w_ocn,
    )
    atm_flux, ocn_flux = pl.pallas_call(
        landing,
        out_shape=(
            jax.ShapeDtypeStruct((owned, nflux, blk), F32),
            jax.ShapeDtypeStruct((waters, nflux, blk), F32),
        ),
        in_specs=[in_vmem] * 4,
        out_specs=[in_vmem] * 2,
        compiler_params=pltpu.CompilerParams(vmem_limit_bytes=LANDING_LIMIT),
    )(*arrived)
    atm_flux = jnp.transpose(atm_flux, (1, 0, 2)).reshape(nflux, owned * blk)
    ocn_flux = jnp.transpose(ocn_flux, (1, 0, 2)).reshape(nflux, waters * blk)
    return (atm_flux, ocn_flux)


def solution(mesh):
    placed = (
        P(None, ("member", "tile")),
        P(None, ("member", "tile", "sub")),
        P(("tile", "sub")),
        P(("tile", "sub")),
        P(("tile", "sub")),
        P(("tile", "sub")),
        P(("tile", "sub")),
        P(("tile", "sub")),
        P(("tile", "sub"), None, None),
        P(("tile", "sub"), None, None),
    )
    return jax.shard_map(
        per_device,
        mesh=mesh,
        in_specs=placed,
        out_specs=(P(None, ("member", "tile")), P(None, ("member", "tile", "sub"))),
        check_vma=False,
    )
```
